32 devices in a mesh: dev: 16 (over z, y, x), rep: 2 (over core).
Axes of the slice: x: 2, y: 2, z: 4, core: 2. Of those that a mesh axis runs over, the one named last changes fastest.
Arguments:
- node_features: bfloat16 [1024, 2, 3136], P('dev', 'rep'), may hold values from -6 to 6
- src_node: int32 [16, 16, 2], P('dev'), may hold values from 0 to 63
- dst_node: int32 [16, 16, 2], P('dev'), may hold values from 0 to 63
- counts: int32 [16, 16], P('dev'), may hold values from 1 to 2, as said below
- rotation: bfloat16 [16, 16, 2, 235], P('dev'), may hold values from -2 to 2
- w_zero: bfloat16 [896, 2, 448], P(None, 'rep'), may hold values from -0.1875 to 0.1875
- w_one: bfloat16 [2, 768, 2, 384], P(None, None, 'rep'), may hold values from -0.15625 to 0.15625
- w_two: bfloat16 [2, 640, 2, 320], P(None, None, 'rep'), may hold values from -0.15625 to 0.15625
- norm_gain: float32 [2, 3136], P('rep'), may hold values from 0.5 to 1.5
Outputs:
- updated: bfloat16 [1024, 2, 3136], P('dev', 'rep')
The draws below stay inside these ranges and needn't reach their ends.
Inputs may be any that keep to these rules, and one draw needn't show every extreme that they name: Slots i < counts[s, d] hold edges, the others padding; in every draw some destination device receives 2 edges from every source device.
All inputs are finite; a program needn't handle non-finite values.
Results may differ from the reference program's by a relative error of at most 0.0054.
Values may be sent and summed in bfloat16 or wider, within the bound.
A program may use at most 64 MiB of HBM per device.

```python
import jax
import jax.numpy as jnp
from jax import lax

C = 128
COEFFS = 49
ROT = 235
NODE_DEV = 64
CAP = 2
CH = 64
NODES = 1024
N_DEV = 16
N_REP = 2


def draw_counts(key, part):
    counts_base = jax.random.randint(jax.random.fold_in(key, 11), (N_DEV, N_DEV), 1, CAP + 1)
    hot_dest = jax.random.randint(jax.random.fold_in(key, 12), (2,), 0, N_DEV)
    column = jnp.arange(N_DEV)
    is_hot = (column[None, :] == hot_dest[0]) | (column[None, :] == hot_dest[1])
    return jnp.where(is_hot, CAP, counts_base).astype(jnp.int32)


def touch_ends(values, key, least, largest):
    longest = values.shape.index(max(values.shape))
    spots = []
    for shift in (0, 1):
        where = [jax.random.randint(jax.random.fold_in(key, axis), (), 0, length) for axis, length in enumerate(values.shape)]
        where[longest] = (where[longest] + shift) % values.shape[longest]
        spots.append(tuple(where))
    return values.at[spots[0]].set(least).at[spots[1]].set(largest)


def block_levels(rng, shape, cuts, least, largest):
    def one(dim, blocks):
        heights = jax.random.uniform(jax.random.fold_in(jax.random.fold_in(rng, 6), dim), (blocks,), jnp.float32, least / len(cuts), largest / len(cuts))
        return jnp.repeat(jnp.exp(heights), shape[dim] // blocks).reshape((-1,) + (1,) * (len(shape) - dim - 1))

    gain = one(*cuts[0])
    for cut in cuts[1:]:
        gain = gain * one(*cut)
    return gain


def centred(own_key, shape, spread, most, cuts=(), dtype=jnp.bfloat16):
    values = spread * jax.random.normal(own_key, shape, jnp.float32)
    if cuts:
        values = values * block_levels(own_key, shape, cuts, -0.22, 0.18)
    return jnp.clip(values, -most, most).astype(dtype)


def setup_inputs(seed: int = 0) -> dict:
    key_list = jax.random.split(jax.random.key(seed), 10)
    return {
        "node_features": centred(key_list[0], (NODES, N_REP, COEFFS * CH), 1.0, 6.0, ((0, 16), (1, 2))),
        "src_node": touch_ends(jax.random.randint(key_list[1], (N_DEV, N_DEV, CAP), 0, NODE_DEV), jax.random.fold_in(key_list[1], 1), 0, NODE_DEV - 1).astype(jnp.int32),
        "dst_node": touch_ends(jax.random.randint(key_list[2], (N_DEV, N_DEV, CAP), 0, NODE_DEV), jax.random.fold_in(key_list[2], 1), 0, NODE_DEV - 1).astype(jnp.int32),
        "counts": draw_counts(jax.random.fold_in(key_list[9], 71), 0),
        "rotation": centred(key_list[4], (N_DEV, N_DEV, CAP, ROT), 0.35, 2.0, ((0, 16),)),
        "w_zero": centred(key_list[5], (7 * C, N_REP, 7 * CH), (7 * C) ** -0.5, 0.1875, ((1, 2),)),
        "w_one": centred(key_list[6], (2, 6 * C, N_REP, 6 * CH), (12 * C) ** -0.5, 0.15625, ((2, 2),)),
        "w_two": centred(key_list[7], (2, 5 * C, N_REP, 5 * CH), (10 * C) ** -0.5, 0.15625, ((2, 2),)),
        "norm_gain": jnp.clip(1.0 + 0.1 * jax.random.normal(key_list[8], (N_REP, COEFFS * CH), jnp.float32), 0.5, 1.5),
    }


def frame_slot(degree, order):
    if order == 0:
        return degree
    if order == 1:
        return 6 + degree
    if order == -1:
        return 12 + degree
    if order == 2:
        return 17 + degree
    return 22 + degree

def frame_tables():
    offsets = []
    places = []
    spot = 0
    for degree in range(7):
        reach = min(degree, 2)
        offsets.append(spot)
        spot += (2 * degree + 1) * (2 * reach + 1)
        places.append([frame_slot(degree, order) for order in range(-reach, reach + 1)])
    return (offsets, places)

def rounded(value):
    return lax.optimization_barrier(value.astype(jnp.bfloat16)).astype(jnp.float32)

def block_of(rotation, offsets, degree):
    reach = min(degree, 2)
    span = 2 * degree + 1
    height = 2 * reach + 1
    piece = rotation[:, offsets[degree]:offsets[degree] + height * span]
    return piece.reshape(rotation.shape[0], height, span).astype(jnp.float32)

def frame(coeffs, rotation):
    offsets, places = frame_tables()
    pieces = []
    for degree in range(7):
        matrix = block_of(rotation, offsets, degree)
        part = coeffs[:, degree * degree:degree * degree + 2 * degree + 1, :].astype(jnp.float32)
        pieces.append(lax.optimization_barrier(jnp.sum(matrix[:, :, :, None] * part[:, None, :, :], axis=2)))
    listing = sorted(((places[degree][row], degree, row) for degree in range(7) for row in range(len(places[degree]))))
    return jnp.concatenate([pieces[degree][:, row:row + 1, :] for place, degree, row in listing], axis=1)

def unframe(framed, rotation):
    offsets, places = frame_tables()
    parts = []
    for degree in range(7):
        matrix = block_of(rotation, offsets, degree)
        chosen = jnp.concatenate([framed[:, place:place + 1, :] for place in places[degree]], axis=1).astype(jnp.float32)
        parts.append(lax.optimization_barrier(jnp.sum(matrix[:, :, :, None] * chosen[:, :, None, :], axis=1)))
    return jnp.concatenate(parts, axis=1)

def mix_orders(rotated, zero_mat, one_mats, two_mats):
    batch = rotated.shape[0]
    out_width = zero_mat.shape[1] // 7
    flat_zero = rotated[:, 0:7, :].reshape(batch, -1)
    result = [jnp.dot(flat_zero, zero_mat, preferred_element_type=jnp.float32).reshape(batch, 7, out_width)]
    for first, count, mats in ((7, 6, one_mats), (19, 5, two_mats)):
        plus = rotated[:, first:first + count, :].reshape(batch, -1)
        minus = rotated[:, first + count:first + 2 * count, :].reshape(batch, -1)
        upper = jnp.dot(plus, mats[0], preferred_element_type=jnp.float32) - jnp.dot(minus, mats[1], preferred_element_type=jnp.float32)
        lower = jnp.dot(plus, mats[1], preferred_element_type=jnp.float32) + jnp.dot(minus, mats[0], preferred_element_type=jnp.float32)
        result.append(upper.reshape(batch, count, out_width))
        result.append(lower.reshape(batch, count, out_width))
    return jnp.concatenate(result, axis=1)

def reference(node_features, src_node, dst_node, counts, rotation, w_zero, w_one, w_two, norm_gain):
    nodes, halves, flat = node_features.shape
    half_width = flat // 49
    width = halves * half_width
    full = node_features.reshape(nodes, halves, 49, half_width).transpose(0, 2, 1, 3).reshape(nodes, 49, width)
    zero_mat = w_zero.reshape(7 * width, halves, 7, half_width).transpose(0, 2, 1, 3).reshape(7 * width, 7 * width)
    one_mats = w_one.reshape(2, 6 * width, halves, 6, half_width).transpose(0, 1, 3, 2, 4).reshape(2, 6 * width, 6 * width)
    two_mats = w_two.reshape(2, 5 * width, halves, 5, half_width).transpose(0, 1, 3, 2, 4).reshape(2, 5 * width, 5 * width)
    slots = jnp.arange(CAP).astype(jnp.int32)
    owners = jnp.arange(N_DEV).astype(jnp.int32)

    def one_source(total, source):
        sources = (source * NODE_DEV + src_node[source].reshape(-1)).astype(jnp.int32)
        gathered = jnp.take(full, sources, axis=0)
        rot_rows = rotation[source].reshape(-1, 235)
        rotated = rounded(frame(gathered, rot_rows)).astype(jnp.bfloat16)
        edge_out = rounded(mix_orders(rotated, zero_mat, one_mats, two_mats))
        back = rounded(unframe(edge_out, rot_rows))
        live = (slots[None, :] < counts[source][:, None]).reshape(-1).astype(jnp.float32)
        back = back * live[:, None, None]
        targets = (owners[:, None] * NODE_DEV + dst_node[:, source, :]).reshape(-1).astype(jnp.int32)
        return (total.at[targets].add(back), None)
    total, unused = lax.scan(one_source, jnp.zeros((nodes, 49, width), jnp.float32), owners)
    mean_sq = lax.optimization_barrier(jnp.sum(total * total, axis=(1, 2))) / (49 * width)
    normed = total * lax.rsqrt(mean_sq + 1e-06)[:, None, None]
    normed = normed.reshape(nodes, 49, halves, half_width).transpose(0, 2, 1, 3).reshape(nodes, halves, flat)
    updated = node_features.astype(jnp.float32) + norm_gain[None].astype(jnp.float32) * normed
    return updated.astype(jnp.bfloat16)
```

```python
import functools

import jax
import jax.numpy as jnp
from jax import lax
from jax.experimental import pallas as pl
from jax.experimental.pallas import tpu as pltpu
from jax.sharding import PartitionSpec as P

LANES = 128
HALF = 64
COEFFS = 49
FRAME = 29
ROT = 235
WINDOW = 120
TILES = (COEFFS + 1) // 2
WIDE = TILES * LANES
MESSAGE = (FRAME + 1) // 2 * LANES
VMEM_LIMIT = 40 * 1024 * 1024
BLOCK = 32
MESH = pl.DeviceIdType.MESH


def frame_slot(degree, order):
    if order == 0:
        return degree
    if order == 1:
        return 6 + degree
    if order == -1:
        return 12 + degree
    if order == 2:
        return 17 + degree
    return 22 + degree


def terms():
    listing = []
    spot = 0
    for degree in range(7):
        reach = min(degree, 2)
        span = 2 * degree + 1
        first = degree * degree
        for row in range(2 * reach + 1):
            slot = frame_slot(degree, row - reach)
            for tile in range(first // 2, (first + span - 1) // 2 + 1):
                ends = []
                for coeff in (2 * tile, 2 * tile + 1):
                    inside = first <= coeff < first + span
                    ends.append(spot + row * span + coeff - first if inside else None)
                listing.append((slot, tile, ends[0], ends[1]))
        spot += span * (2 * reach + 1)
    return listing


TERMS = terms()


def message_place(slot):
    return slot // 2, slot % 2


def far_first(count):
    return sorted(range(1, count), key=lambda offset: -min(offset, count - offset))


def each_peer(count, func):
    if count <= 17:
        for offset in far_first(count):
            func(offset - 1)
    else:
        each(count - 1, func)


def each(count, func):
    if count <= 16:
        for index in range(count):
            func(index)
    else:
        lax.fori_loop(0, count, lambda index, carry: (func(index), carry)[1], 0)


def kernel(
    peers,
    slots,
    x_hbm,
    rot_hbm,
    src_hbm,
    cnt_hbm,
    dst_hbm,
    gain_hbm,
    w0_hbm,
    w1_hbm,
    w2_hbm,
    out_ref,
    x_ref,
    rot_ref,
    src_ref,
    cnt_ref,
    dst_ref,
    gain_ref,
    w0,
    w1,
    w2,
    low_scr,
    high_scr,
    xg,
    own,
    packed,
    other,
    lhs,
    y_scr,
    msg,
    recv,
    rrot,
    mult,
    f_scr,
    back,
    total,
    sq,
    sq_other,
    wsem,
    esem,
    rot_sem,
    msg_sem,
    qsem,
):
    me = lax.axis_index("dev")
    half = lax.axis_index("rep")
    nodes = x_ref.shape[0]
    flat = x_ref.shape[1]
    blocks = peers * slots // BLOCK
    group = BLOCK // slots
    partner = {"rep": 1 - half}

    def peer(offset):
        return lax.rem(me + offset, peers)

    loads = [
        pltpu.make_async_copy(src, dst, wsem.at[index])
        for index, (src, dst) in enumerate(
            (
                (x_hbm, x_ref),
                (rot_hbm, rot_ref),
                (src_hbm, src_ref),
                (cnt_hbm, cnt_ref),
                (dst_hbm, dst_ref),
                (gain_hbm, gain_ref),
                (w0_hbm, w0),
                (w1_hbm, w1),
                (w2_hbm, w2),
            )
        )
    ]
    for copy in loads:
        copy.start()
    barrier = pltpu.get_barrier_semaphore()
    pl.semaphore_signal(barrier, inc=1, device_id=partner, device_id_type=MESH)
    each(
        peers - 1,
        lambda o: pl.semaphore_signal(
            barrier, inc=1, device_id={"dev": peer(o + 1)}, device_id_type=MESH
        ),
    )

    lane = lax.broadcasted_iota(jnp.int32, (BLOCK, LANES), 1)
    low_half = lane < HALF
    mine = (lane // HALF) == half

    y_scr[...] = jnp.zeros_like(y_scr)
    xg[:, (TILES - 1) * LANES :] = jnp.zeros((BLOCK, LANES), jnp.float32)
    low_scr[...] = jnp.zeros_like(low_scr)
    high_scr[...] = jnp.zeros_like(high_scr)

    def column(rows):
        row = lax.broadcasted_iota(jnp.int32, (BLOCK, group), 0)
        spot = lax.broadcasted_iota(jnp.int32, (BLOCK, group), 1)
        chosen = jnp.zeros((BLOCK, group), jnp.float32)
        for index in range(slots):
            chosen = jnp.where(row == spot * slots + index, rows[index], chosen)
        return jnp.sum(chosen, axis=1, keepdims=True)

    def sources(block):
        count = cnt_ref[block]
        value = src_ref[block]
        return column(
            [
                jnp.where(count > index, value[index : index + 1], -1).astype(jnp.float32)
                for index in range(slots)
            ]
        )

    def targets(block):
        value = dst_ref[block].astype(jnp.float32)
        down = column([value[index : index + 1] for index in range(slots)])
        row = lax.broadcasted_iota(jnp.int32, (BLOCK, BLOCK), 0)
        spot = lax.broadcasted_iota(jnp.int32, (BLOCK, BLOCK), 1)
        return jnp.sum(jnp.where(row == spot, down, 0.0), axis=0, keepdims=True)

    def load_rotation(ref, start):
        for index in range(group):
            rows = ref[start + index].astype(jnp.float32)
            low_scr[index * slots : (index + 1) * slots, 0:WINDOW] = rows[:, 0:WINDOW]
            high_scr[index * slots : (index + 1) * slots, 0:WINDOW] = rows[:, ROT - WINDOW :]
        return low_scr[...], high_scr[...]

    def multiplier(tables, first, second):
        given = [entry for entry in (first, second) if entry is not None]
        which = 0 if max(given) < WINDOW else 1
        shift = which * (ROT - WINDOW)
        places = [WINDOW if e is None else e - shift for e in (first, second)]
        index = jnp.where(low_half, places[0], places[1])
        return jnp.take_along_axis(tables[which], index, axis=1, mode="promise_in_bounds")

    def turn(block):
        tables = load_rotation(rot_ref, block * group)
        hot = (
            lax.broadcasted_iota(jnp.int32, (BLOCK, nodes), 1).astype(jnp.float32) == sources(block)
        ).astype(jnp.bfloat16)
        xg[:, 0:flat] = jnp.dot(hot, x_ref[...], preferred_element_type=jnp.float32)
        sums = [None] * FRAME
        for slot, tile, first, second in TERMS:
            part = multiplier(tables, first, second) * xg[:, tile * LANES : (tile + 1) * LANES]
            sums[slot] = part if sums[slot] is None else sums[slot] + part
        for slot in range(FRAME):
            sums[slot] = sums[slot] + pltpu.roll(sums[slot], HALF, 1)
            own[block, :, slot * LANES : (slot + 1) * LANES] = sums[slot]
        for pair in range((FRAME + 1) // 2):
            first = sums[2 * pair]
            second = sums[min(2 * pair + 1, FRAME - 1)]
            packed[block, :, pair * LANES : (pair + 1) * LANES] = jnp.where(
                mine, first, second
            ).astype(jnp.bfloat16)

    for copy in loads[:4]:
        copy.wait()
    each(blocks, turn)

    pl.semaphore_wait(barrier, peers)

    exchange = pltpu.make_async_remote_copy(
        src_ref=packed,
        dst_ref=other,
        send_sem=esem.at[0],
        recv_sem=esem.at[1],
        device_id=partner,
        device_id_type=MESH,
    )
    exchange.start()

    def transfer(source, target, send, receive, o):
        to = peer(o + 1)
        return pltpu.make_async_remote_copy(
            src_ref=source.at[to],
            dst_ref=target.at[me],
            send_sem=send,
            recv_sem=receive,
            device_id={"dev": to},
            device_id_type=MESH,
        )

    def rotations(o):
        return transfer(rot_ref, rrot, rot_sem.at[0], rot_sem.at[1], o)

    def messages(o):
        return transfer(msg, recv, msg_sem.at[0], msg_sem.at[1], o)

    def everything(source, target, sems):
        return pltpu.make_async_remote_copy(
            src_ref=source.at[pl.ds(0, peers - 1)],
            dst_ref=target.at[pl.ds(0, peers - 1)],
            send_sem=sems.at[0],
            recv_sem=sems.at[1],
            device_id={"dev": peer(1)},
            device_id_type=MESH,
        )

    all_rotations = everything(rot_ref, rrot, rot_sem)
    all_messages = everything(msg, recv, msg_sem)

    each_peer(peers, lambda o: rotations(o).start())
    rrot[me] = rot_ref[me]

    for copy in loads[4:]:
        copy.wait()
    exchange.wait()

    def mix(block):
        for pair in range((FRAME + 1) // 2):
            there = other[block, :, pair * LANES : (pair + 1) * LANES].astype(jnp.float32)
            for slot, value in ((2 * pair, there), (2 * pair + 1, None)):
                if slot < FRAME:
                    value = pltpu.roll(there, HALF, 1) if value is None else value
                    cols = slice(slot * LANES, (slot + 1) * LANES)
                    lhs[:, cols] = jnp.where(mine, own[block, :, cols], value).astype(jnp.bfloat16)
        nt = (((1,), (1,)), ((), ()))
        y_scr[:, 0 : 7 * HALF] = lax.dot_general(
            lhs[:, 0 : 7 * LANES], w0[...], nt, preferred_element_type=jnp.float32
        )
        for start, count, ref, dims in (
            (7, 6, w1, (((1,), (0,)), ((), ()))),
            (19, 5, w2, nt),
        ):
            rows = jnp.concatenate(
                [
                    lhs[:, start * LANES : (start + count) * LANES],
                    lhs[:, (start + count) * LANES : (start + 2 * count) * LANES],
                ],
                axis=0,
            )
            real = lax.dot_general(rows, ref[0], dims, preferred_element_type=jnp.float32)
            imag = lax.dot_general(rows, ref[1], dims, preferred_element_type=jnp.float32)
            width = count * HALF
            plus = start * HALF
            minus = plus + width
            y_scr[:, plus : plus + width] = real[:BLOCK] - imag[BLOCK:]
            y_scr[:, minus : minus + width] = imag[:BLOCK] + real[BLOCK:]
        for index in range(group):
            msg[block * group + index] = y_scr[index * slots : (index + 1) * slots, :].astype(
                jnp.bfloat16
            )

    each(blocks, mix)
    each_peer(peers, lambda o: messages(o).start())
    recv[me] = msg[me]

    all_rotations.wait_recv()

    def prepare(block):
        tables = load_rotation(rrot, block * group)
        for number, (slot, tile, first, second) in enumerate(TERMS):
            mult[number] = multiplier(tables, first, second)

    def collect(block, add):
        for index in range(group):
            f_scr[index * slots : (index + 1) * slots, :] = recv[block * group + index].astype(
                jnp.float32
            )
        doubled = {}
        for slot in range(FRAME):
            tile, side = message_place(slot)
            value = f_scr[:, tile * LANES : (tile + 1) * LANES]
            turned = pltpu.roll(value, HALF, 1)
            doubled[slot] = (
                jnp.where(low_half, value, turned) if side == 0 else jnp.where(low_half, turned, value)
            )
        sums = [None] * TILES
        for number, (slot, tile, first, second) in enumerate(TERMS):
            part = mult[number] * doubled[slot]
            sums[tile] = part if sums[tile] is None else sums[tile] + part
        for tile in range(TILES):
            back[:, tile * LANES : (tile + 1) * LANES] = sums[tile].astype(jnp.bfloat16)
        hot = (
            lax.broadcasted_iota(jnp.int32, (nodes, BLOCK), 0).astype(jnp.float32) == targets(block)
        ).astype(jnp.bfloat16)
        value = jnp.dot(hot, back[...], preferred_element_type=jnp.float32)
        total[...] = total[...] + value if add else value

    if blocks == 1:
        prepare(0)
        all_messages.wait_recv()
        collect(0, False)
    else:
        all_messages.wait_recv()
        total[...] = jnp.zeros_like(total)

        def one(block, carry):
            prepare(block)
            collect(block, True)
            return carry

        lax.fori_loop(0, blocks, one, 0)

    partial = None
    for tile in range(TILES):
        value = total[:, tile * LANES : (tile + 1) * LANES]
        partial = value * value if partial is None else partial + value * value
    sq[...] = partial
    share = pltpu.make_async_remote_copy(
        src_ref=sq,
        dst_ref=sq_other,
        send_sem=qsem.at[0],
        recv_sem=qsem.at[1],
        device_id=partner,
        device_id_type=MESH,
    )
    share.start()
    all_rotations.wait_send()
    all_messages.wait_send()
    share.wait()
    mean_sq = jnp.sum(sq[...] + sq_other[...], axis=1, keepdims=True) / (2 * flat)
    scale = lax.rsqrt(mean_sq + 1e-06)
    for start in range(0, flat, LANES):
        cols = slice(start, min(start + LANES, flat))
        normed = total[:, cols] * scale
        out_ref[:, cols] = (
            x_ref[:, cols].astype(jnp.float32) + gain_ref[:, cols] * normed
        ).astype(jnp.bfloat16)


def shards(node_features, src_node, dst_node, counts, rotation, w_zero, w_one, w_two, norm_gain):
    nodes, _, flat = node_features.shape
    peers, slots = src_node.shape[1:]
    edges = peers * slots
    blocks = edges // BLOCK
    x = node_features.reshape(nodes, flat)
    group = peers // blocks
    src = src_node.reshape(blocks, group, slots).swapaxes(1, 2)
    dst = dst_node.reshape(blocks, group, slots).swapaxes(1, 2)
    cnt = counts.reshape(blocks, 1, group)
    rot = rotation.reshape(peers, slots, ROT)
    w0 = w_zero.reshape(w_zero.shape[0], -1).T
    w1 = w_one.reshape(2, w_one.shape[1], -1)
    w2 = w_two.reshape(2, w_two.shape[1], -1).swapaxes(1, 2)
    vmem = pl.BlockSpec(memory_space=pltpu.VMEM)
    hbm = pl.BlockSpec(memory_space=pltpu.HBM)
    f32, bf16 = jnp.float32, jnp.bfloat16
    dma = pltpu.SemaphoreType.DMA
    pairs = (FRAME + 1) // 2
    operands = (x, rot, src, cnt, dst, norm_gain, w0, w1, w2)
    out = pl.pallas_call(
        functools.partial(kernel, peers, slots),
        out_shape=jax.ShapeDtypeStruct((nodes, flat), bf16),
        in_specs=[hbm] * 9,
        out_specs=vmem,
        scratch_shapes=[
            pltpu.VMEM(x.shape, bf16),
            pltpu.VMEM(rot.shape, bf16),
            pltpu.VMEM(src.shape, jnp.int32),
            pltpu.VMEM(cnt.shape, jnp.int32),
            pltpu.VMEM(dst.shape, jnp.int32),
            pltpu.VMEM(norm_gain.shape, f32),
            pltpu.VMEM(w0.shape, bf16),
            pltpu.VMEM(w1.shape, bf16),
            pltpu.VMEM(w2.shape, bf16),
            pltpu.VMEM((BLOCK, LANES), f32),
            pltpu.VMEM((BLOCK, LANES), f32),
            pltpu.VMEM((BLOCK, WIDE), f32),
            pltpu.VMEM((blocks, BLOCK, FRAME * LANES), f32),
            pltpu.VMEM((blocks, BLOCK, pairs * LANES), bf16),
            pltpu.VMEM((blocks, BLOCK, pairs * LANES), bf16),
            pltpu.VMEM((BLOCK, FRAME * LANES), bf16),
            pltpu.VMEM((BLOCK, MESSAGE), f32),
            pltpu.VMEM((peers, slots, MESSAGE), bf16),
            pltpu.VMEM((peers, slots, MESSAGE), bf16),
            pltpu.VMEM((peers, slots, ROT), bf16),
            pltpu.VMEM((len(TERMS), BLOCK, LANES), f32),
            pltpu.VMEM((BLOCK, MESSAGE), f32),
            pltpu.VMEM((BLOCK, WIDE), bf16),
            pltpu.VMEM((nodes, WIDE), f32),
            pltpu.VMEM((nodes, LANES), f32),
            pltpu.VMEM((nodes, LANES), f32),
            dma((9,)),
            dma((2,)),
            dma((2,)),
            dma((2,)),
            dma((2,)),
        ],
        compiler_params=pltpu.CompilerParams(
            collective_id=0, has_side_effects=True, vmem_limit_bytes=VMEM_LIMIT
        ),
    )(*(pltpu.with_memory_space_constraint(operand, pltpu.HBM) for operand in operands))
    return out.reshape(nodes, 1, flat)


def solution(mesh):
    return jax.shard_map(
        shards,
        mesh=mesh,
        in_specs=(
            P("dev", "rep", None),
            P("dev", None, None),
            P("dev", None, None),
            P("dev", None),
            P("dev", None, None, None),
            P(None, "rep", None),
            P(None, None, "rep", None),
            P(None, None, "rep", None),
            P("rep", None),
        ),
        out_specs=P("dev", "rep", None),
        check_vma=False,
    )
```

```python
import functools

import jax
import jax.numpy as jnp
from jax import lax
from jax.experimental import pallas as pl
from jax.experimental.pallas import tpu as pltpu
from jax.sharding import PartitionSpec as P

LANES = 128
HALF = 64
COEFFS = 49
FRAME = 29
ROT = 235
TILES = (COEFFS + 1) // 2
WIDE = TILES * LANES
MESSAGE = (FRAME + 1) // 2 * LANES
VMEM_LIMIT = 40 * 1024 * 1024
BLOCK = 32
MESH = pl.DeviceIdType.MESH
ORDERS = ((0, 7), (7, 6), (13, 6), (19, 5), (24, 5))
SEND_ORDER = (0, 4, 1, 2, 3)


def frame_slot(degree, order):
    if order == 0:
        return degree
    if order == 1:
        return 6 + degree
    if order == -1:
        return 12 + degree
    if order == 2:
        return 17 + degree
    return 22 + degree


def listings():
    groups = []
    parts = []
    segments = []
    spot = 0
    for degree in range(7):
        reach = min(degree, 2)
        span = 2 * degree + 1
        first = degree * degree
        for row in range(2 * reach + 1):
            slot = frame_slot(degree, row - reach)
            base = spot + row * span - first
            segments.append((base + first, (-base) % 4))
            for quad in range(first // 4, (first + span - 1) // 4 + 1):
                low = base + max(4 * quad, first)
                high = base + min(4 * quad + 3, first + span - 1)
                for window in (0, 1):
                    start = max(low, window * LANES)
                    end = min(high, window * LANES + LANES - 1)
                    if start <= end:
                        for which in (0, 1):
                            tile = 2 * quad + which
                            if any((e - base) // 2 == tile for e in range(start, end + 1)):
                                parts.append((slot, tile, len(groups), which))
                        groups.append((window, start, end))
        spot += span * (2 * reach + 1)
    return groups, parts, segments


GROUPS, PARTS, SEGMENTS = listings()
LOW_ROWS = BLOCK * sum(window == 0 for window, _, _ in GROUPS)
ALL_ROWS = BLOCK * len(GROUPS)


def packed_pairs():
    pairs = []
    starts = []
    for first, count in ORDERS:
        starts.append(len(pairs) * LANES)
        for slot in range(first, first + count, 2):
            pairs.append((slot, min(slot + 1, first + count - 1)))
    return pairs, starts


PAIRS, STARTS = packed_pairs()


def message_starts():
    starts = {}
    spot = 0
    for order in SEND_ORDER:
        starts[order] = spot
        spot += ORDERS[order][1] * HALF
    return starts


SENT = message_starts()
SPLIT = (ORDERS[3][1] + 1) // 2 * LANES


def message_place(slot):
    order = max(o for o, (first, _) in enumerate(ORDERS) if first <= slot)
    place = SENT[order] // HALF + slot - ORDERS[order][0]
    return place // 2, place % 2


def far_first(count):
    return sorted(range(1, count), key=lambda offset: -min(offset, count - offset))


def each_peer(count, func):
    if count <= 17:
        for offset in far_first(count):
            func(offset - 1)
    else:
        each(count - 1, func)


def each(count, func):
    if count <= 16:
        for index in range(count):
            func(index)
    else:
        lax.fori_loop(0, count, lambda index, carry: (func(index), carry)[1], 0)


def kernel(
    peers,
    slots,
    x_hbm,
    rot_hbm,
    src_hbm,
    cnt_hbm,
    dst_hbm,
    w0_hbm,
    w1_hbm,
    w2_hbm,
    x_ref,
    total,
    sums_ref,
    rot_ref,
    src_ref,
    cnt_ref,
    dst_ref,
    w0_raw,
    w2_raw,
    w0,
    w1,
    w2,
    expand,
    rot_scr,
    entries,
    mult,
    xg,
    turned,
    part_scr,
    y_scr,
    msg,
    recv,
    rrot,
    f_scr,
    back,
    sq,
    sq_other,
    wsem,
    esem,
    rot_sem,
    msg_sem,
    qsem,
):
    me = lax.axis_index("dev")
    half = lax.axis_index("rep")
    nodes = x_ref.shape[0]
    flat = x_ref.shape[1]
    blocks = peers * slots // BLOCK
    group = BLOCK // slots
    partner = {"rep": 1 - half}

    def peer(offset):
        return lax.rem(me + offset, peers)

    def load(index, src, dst):
        return pltpu.make_async_copy(src, dst, wsem.at[index])

    early = [
        load(0, rot_hbm, rot_ref),
        load(1, src_hbm, src_ref),
        load(2, cnt_hbm, cnt_ref),
        load(3, x_hbm, x_ref),
    ]
    late = [load(4, dst_hbm, dst_ref), load(5, w0_hbm, w0_raw), load(6, w2_hbm, w2_raw)]
    width = w1_hbm.shape[-1]
    for side in (0, 1):
        for kind in (0, 1):
            cols = slice(kind * width, (kind + 1) * width)
            late.append(load(7, w1_hbm.at[kind, :, side], w1.at[side, :, :, cols]))
    waits = late[:3] + [load(7, w1, w1)]
    for copy in early + late:
        copy.start()
    barrier = pltpu.get_barrier_semaphore()
    pl.semaphore_signal(barrier, inc=1, device_id=partner, device_id_type=MESH)
    each(
        peers - 1,
        lambda o: pl.semaphore_signal(
            barrier, inc=1, device_id={"dev": peer(o + 1)}, device_id_type=MESH
        ),
    )

    lane = lax.broadcasted_iota(jnp.int32, (BLOCK, LANES), 1)
    low_half = lane < HALF

    y_scr[...] = jnp.zeros_like(y_scr)
    xg[:, flat:] = jnp.zeros((BLOCK, xg.shape[1] - flat), jnp.float32)
    for window in (0, 1):
        entry = lax.broadcasted_iota(jnp.int32, (LANES, LANES), 0) + window * LANES
        spot = lax.broadcasted_iota(jnp.int32, (LANES, LANES), 1)
        shift = jnp.zeros_like(entry)
        for start, offset in SEGMENTS:
            shift = jnp.where(entry >= start, offset, shift)
        place = lax.rem(entry + shift, 4)
        for side in (0, 1):
            hit = place == lax.div(spot, HALF) + 2 * side
            expand[window, :, side * LANES : (side + 1) * LANES] = jnp.where(
                hit, 1.0, 0.0
            ).astype(jnp.bfloat16)

    def column(rows):
        row = lax.broadcasted_iota(jnp.int32, (BLOCK, group), 0)
        spot = lax.broadcasted_iota(jnp.int32, (BLOCK, group), 1)
        chosen = jnp.zeros((BLOCK, group), jnp.float32)
        for index in range(slots):
            chosen = jnp.where(row == spot * slots + index, rows[index], chosen)
        return jnp.sum(chosen, axis=1, keepdims=True)

    def sources(block):
        count = cnt_ref[block]
        value = src_ref[block]
        return column(
            [
                jnp.where(count > index, value[index : index + 1], -1).astype(jnp.float32)
                for index in range(slots)
            ]
        )

    def targets(block):
        value = dst_ref[block].astype(jnp.float32)
        down = column([value[index : index + 1] for index in range(slots)])
        row = lax.broadcasted_iota(jnp.int32, (BLOCK, BLOCK), 0)
        spot = lax.broadcasted_iota(jnp.int32, (BLOCK, BLOCK), 1)
        return jnp.sum(jnp.where(row == spot, down, 0.0), axis=0, keepdims=True)

    def spread(ref, start):
        for index in range(group):
            rot_scr[index * slots : (index + 1) * slots, 0:ROT] = ref[start + index].astype(
                jnp.float32
            )
        for number, (window, first, last) in enumerate(GROUPS):
            spots = lane + window * LANES
            rows = rot_scr[:, window * LANES : (window + 1) * LANES]
            entries[number * BLOCK : (number + 1) * BLOCK, :] = jnp.where(
                (spots >= first) & (spots <= last), rows, 0.0
            ).astype(jnp.bfloat16)
        for window, rows in enumerate((slice(0, LOW_ROWS), slice(LOW_ROWS, ALL_ROWS))):
            mult[rows] = jnp.dot(
                entries[rows], expand[window], preferred_element_type=jnp.float32
            )

    def factor(number, which):
        return mult[number * BLOCK : (number + 1) * BLOCK, which * LANES : (which + 1) * LANES]

    def turn(block):
        spread(rot_ref, block * group)
        if block is first_block:
            for copy in early[1:]:
                copy.wait()
        hot = (
            lax.broadcasted_iota(jnp.int32, (BLOCK, nodes), 1).astype(jnp.float32) == sources(block)
        ).astype(jnp.bfloat16)
        xg[:, 0:flat] = jnp.dot(hot, x_ref[...], preferred_element_type=jnp.float32)
        sums = [None] * FRAME
        for slot, tile, number, which in PARTS:
            part = factor(number, which) * xg[:, tile * LANES : (tile + 1) * LANES]
            sums[slot] = part if sums[slot] is None else sums[slot] + part
        for pair, (one, two) in enumerate(PAIRS):
            kept = jnp.where(low_half, sums[one], sums[two])
            moved = jnp.where(low_half, sums[two], sums[one])
            turned[half, block, :, pair * LANES : (pair + 1) * LANES] = (
                kept + pltpu.roll(moved, HALF, 1)
            ).astype(jnp.bfloat16)

    early[0].wait()
    first_block = 0 if blocks <= 16 else None
    if first_block is None:
        for copy in early[1:]:
            copy.wait()
    each(blocks, turn)

    pl.semaphore_wait(barrier, peers)

    exchange = pltpu.make_async_remote_copy(
        src_ref=turned.at[half],
        dst_ref=turned.at[half],
        send_sem=esem.at[0],
        recv_sem=esem.at[1],
        device_id=partner,
        device_id_type=MESH,
    )
    exchange.start()

    def transfer(source, target, send, receive, o):
        to = peer(o + 1)
        return pltpu.make_async_remote_copy(
            src_ref=source.at[to],
            dst_ref=target.at[me],
            send_sem=send,
            recv_sem=receive,
            device_id={"dev": to},
            device_id_type=MESH,
        )

    def rotations(o):
        return transfer(rot_ref, rrot, rot_sem.at[0], rot_sem.at[1], o)

    def messages(o):
        return transfer(msg, recv, msg_sem.at[0], msg_sem.at[1], o)

    def everything(source, target, sems):
        return pltpu.make_async_remote_copy(
            src_ref=source.at[pl.ds(0, peers - 1)],
            dst_ref=target.at[pl.ds(0, peers - 1)],
            send_sem=sems.at[0],
            recv_sem=sems.at[1],
            device_id={"dev": peer(1)},
            device_id_type=MESH,
        )

    all_rotations = everything(rot_ref, rrot, rot_sem)
    all_messages = everything(msg, recv, msg_sem)

    each_peer(peers, lambda o: rotations(o).start())
    rrot[me] = rot_ref[me]

    for copy in waits:
        copy.wait()
    for slot in range(ORDERS[0][1]):
        flipped = w0_raw[:, slot * LANES : (slot + 1) * LANES].T
        for side in (0, 1):
            w0[side, slot * HALF : (slot + 1) * HALF, :] = flipped[side * HALF : (side + 1) * HALF]
    for kind in (0, 1):
        for slot in range(ORDERS[3][1]):
            flipped = w2_raw[kind, :, slot * LANES : (slot + 1) * LANES].T
            for side in (0, 1):
                w2[
                    side,
                    slot * HALF : (slot + 1) * HALF,
                    kind * SPLIT : kind * SPLIT + flipped.shape[1],
                ] = flipped[side * HALF : (side + 1) * HALF]

    def product(side, block):
        def rows(order):
            start = STARTS[order]
            return turned[side, block, :, start : start + ORDERS[order][1] * HALF]

        def dot(lhs, rhs):
            return jnp.dot(lhs, rhs, preferred_element_type=jnp.float32)

        results = [dot(rows(0), w0[side])]
        for plus, ref, gap in ((1, w1, width), (3, w2, SPLIT)):
            pair = jnp.concatenate([rows(plus), rows(plus + 1)], axis=0)
            weights = ref[side]
            if weights.ndim == 3:
                weights = weights.reshape(-1, weights.shape[-1])
            both = dot(pair, weights)
            span = ORDERS[plus][1] * HALF
            results.append(both[:BLOCK, :span] - both[BLOCK:, gap : gap + span])
            results.append(both[:BLOCK, gap : gap + span] + both[BLOCK:, :span])
        return results

    def own(block):
        for order, value in enumerate(product(half, block)):
            start = STARTS[order]
            part_scr[block, :, start : start + value.shape[1]] = value

    def mix(block):
        for order, value in enumerate(product(1 - half, block)):
            start = STARTS[order]
            sent = SENT[order]
            y_scr[:, sent : sent + value.shape[1]] = (
                value + part_scr[block, :, start : start + value.shape[1]]
            )
        for index in range(group):
            msg[block * group + index] = y_scr[index * slots : (index + 1) * slots, :].astype(
                jnp.bfloat16
            )

    each(blocks, own)
    exchange.wait()
    each(blocks, mix)
    each_peer(peers, lambda o: messages(o).start())
    recv[me] = msg[me]

    all_rotations.wait_recv()

    def prepare(block):
        spread(rrot, block * group)

    def collect(block, add):
        for index in range(group):
            f_scr[index * slots : (index + 1) * slots, :] = recv[block * group + index].astype(
                jnp.float32
            )
        doubled = {}
        for slot in range(FRAME):
            tile, side = message_place(slot)
            value = f_scr[:, tile * LANES : (tile + 1) * LANES]
            turned = pltpu.roll(value, HALF, 1)
            doubled[slot] = (
                jnp.where(low_half, value, turned) if side == 0 else jnp.where(low_half, turned, value)
            )
        sums = [None] * TILES
        for slot, tile, number, which in PARTS:
            part = factor(number, which) * doubled[slot]
            sums[tile] = part if sums[tile] is None else sums[tile] + part
        for tile in range(TILES):
            back[:, tile * LANES : (tile + 1) * LANES] = sums[tile].astype(jnp.bfloat16)
        hot = (
            lax.broadcasted_iota(jnp.int32, (nodes, BLOCK), 0).astype(jnp.float32) == targets(block)
        ).astype(jnp.bfloat16)
        value = jnp.dot(hot, back[...], preferred_element_type=jnp.float32)
        total[...] = total[...] + value if add else value

    if blocks == 1:
        prepare(0)
        all_messages.wait_recv()
        collect(0, False)
    else:
        all_messages.wait_recv()
        total[...] = jnp.zeros_like(total)

        def one(block, carry):
            prepare(block)
            collect(block, True)
            return carry

        lax.fori_loop(0, blocks, one, 0)

    partial = None
    for tile in range(TILES):
        value = total[:, tile * LANES : (tile + 1) * LANES]
        partial = value * value if partial is None else partial + value * value
    sq[...] = partial
    share = pltpu.make_async_remote_copy(
        src_ref=sq,
        dst_ref=sq_other,
        send_sem=qsem.at[0],
        recv_sem=qsem.at[1],
        device_id=partner,
        device_id_type=MESH,
    )
    share.start()
    all_rotations.wait_send()
    all_messages.wait_send()
    share.wait()
    sums_ref[...] = sq[...] + sq_other[...]


def finish(chunks, x_ref, total, sums_ref, gain_ref, out_hbm, out_ref, sems):
    flat = x_ref.shape[1]
    mean_sq = jnp.sum(sums_ref[...], axis=1, keepdims=True) / (2 * flat)
    scale = lax.rsqrt(mean_sq + 1e-06)
    copies = []
    for index, (first, last) in enumerate(chunks):
        for start in range(first, last, LANES):
            cols = slice(start, min(start + LANES, last))
            normed = total[:, cols] * scale
            out_ref[:, cols] = (
                x_ref[:, cols].astype(jnp.float32) + gain_ref[:, cols] * normed
            ).astype(jnp.bfloat16)
        part = slice(first, last)
        copies.append(
            pltpu.make_async_copy(out_ref.at[:, part], out_hbm.at[:, part], sems.at[index])
        )
        copies[-1].start()
    for copy in copies:
        copy.wait()


def shards(node_features, src_node, dst_node, counts, rotation, w_zero, w_one, w_two, norm_gain):
    nodes, _, flat = node_features.shape
    peers, slots = src_node.shape[1:]
    edges = peers * slots
    blocks = edges // BLOCK
    x = node_features.reshape(nodes, flat)
    group = peers // blocks
    src = src_node.reshape(blocks, group, slots).swapaxes(1, 2)
    dst = dst_node.reshape(blocks, group, slots).swapaxes(1, 2)
    cnt = counts.reshape(blocks, 1, group)
    rot = rotation.reshape(peers, slots, ROT)
    w0 = w_zero.reshape(w_zero.shape[0], -1).T
    w1 = w_one.reshape(2, -1, 2, HALF, w_one.shape[-1])
    w2 = w_two.reshape(2, w_two.shape[1], -1).swapaxes(1, 2)
    vmem = pl.BlockSpec(memory_space=pltpu.VMEM)
    hbm = pl.BlockSpec(memory_space=pltpu.HBM)
    f32, bf16 = jnp.float32, jnp.bfloat16
    dma = pltpu.SemaphoreType.DMA
    operands = (x, rot, src, cnt, dst, w0, w1, w2)
    held, total, sums = pl.pallas_call(
        functools.partial(kernel, peers, slots),
        out_shape=(
            jax.ShapeDtypeStruct((nodes, flat), bf16),
            jax.ShapeDtypeStruct((nodes, WIDE), f32),
            jax.ShapeDtypeStruct((nodes, LANES), f32),
        ),
        in_specs=[hbm] * 8,
        out_specs=(vmem,) * 3,
        scratch_shapes=[
            pltpu.VMEM(rot.shape, bf16),
            pltpu.VMEM(src.shape, jnp.int32),
            pltpu.VMEM(cnt.shape, jnp.int32),
            pltpu.VMEM(dst.shape, jnp.int32),
            pltpu.VMEM(w0.shape, bf16),
            pltpu.VMEM(w2.shape, bf16),
            pltpu.VMEM((2, w0.shape[1] // 2, w0.shape[0]), bf16),
            pltpu.VMEM((2, w1.shape[1], HALF, 2 * w1.shape[-1]), bf16),
            pltpu.VMEM((2, w2.shape[2] // 2, 2 * SPLIT), bf16),
            pltpu.VMEM((2, LANES, 2 * LANES), bf16),
            pltpu.VMEM((BLOCK, 2 * LANES), f32),
            pltpu.VMEM((ALL_ROWS, LANES), bf16),
            pltpu.VMEM((ALL_ROWS, 2 * LANES), f32),
            pltpu.VMEM((BLOCK, WIDE), f32),
            pltpu.VMEM((2, blocks, BLOCK, len(PAIRS) * LANES), bf16),
            pltpu.VMEM((blocks, BLOCK, len(PAIRS) * LANES), f32),
            pltpu.VMEM((BLOCK, MESSAGE), f32),
            pltpu.VMEM((peers, slots, MESSAGE), bf16),
            pltpu.VMEM((peers, slots, MESSAGE), bf16),
            pltpu.VMEM((peers, slots, ROT), bf16),
            pltpu.VMEM((BLOCK, MESSAGE), f32),
            pltpu.VMEM((BLOCK, WIDE), bf16),
            pltpu.VMEM((nodes, LANES), f32),
            pltpu.VMEM((nodes, LANES), f32),
            dma((8,)),
            dma((2,)),
            dma((2,)),
            dma((2,)),
            dma((2,)),
        ],
        compiler_params=pltpu.CompilerParams(
            collective_id=0, has_side_effects=True, vmem_limit_bytes=VMEM_LIMIT
        ),
    )(*(pltpu.with_memory_space_constraint(operand, pltpu.HBM) for operand in operands))
    cut = (flat // LANES + 3) // 4 * LANES
    chunks = [(start, min(start + cut, flat)) for start in range(0, flat, cut)]
    out = pl.pallas_call(
        functools.partial(finish, chunks),
        out_shape=jax.ShapeDtypeStruct((nodes, flat), bf16),
        in_specs=[vmem] * 4,
        out_specs=hbm,
        scratch_shapes=[pltpu.VMEM((nodes, flat), bf16), dma((len(chunks),))],
        compiler_params=pltpu.CompilerParams(vmem_limit_bytes=VMEM_LIMIT),
    )(held, total, sums, norm_gain)
    return out.reshape(nodes, 1, flat)


def solution(mesh):
    return jax.shard_map(
        shards,
        mesh=mesh,
        in_specs=(
            P("dev", "rep", None),
            P("dev", None, None),
            P("dev", None, None),
            P("dev", None),
            P("dev", None, None, None),
            P(None, "rep", None),
            P(None, None, "rep", None),
            P(None, None, "rep", None),
            P("rep", None),
        ),
        out_specs=P("dev", "rep", None),
        check_vma=False,
    )
```

```python
import functools

import jax
import jax.numpy as jnp
from jax import lax
from jax.experimental import pallas as pl
from jax.experimental.pallas import tpu as pltpu
from jax.sharding import PartitionSpec as P

LANES = 128
HALF = 64
COEFFS = 49
FRAME = 29
ROT = 235
TILES = (COEFFS + 1) // 2
WIDE = TILES * LANES
MESSAGE = (FRAME + 1) // 2 * LANES
VMEM_LIMIT = 40 * 1024 * 1024
BLOCK = 32
PIECE = 16
MESH = pl.DeviceIdType.MESH
ORDERS = ((0, 7), (7, 6), (13, 6), (19, 5), (24, 5))
SEND_ORDER = (0, 4, 1, 2, 3)


def frame_slot(degree, order):
    if order == 0:
        return degree
    if order == 1:
        return 6 + degree
    if order == -1:
        return 12 + degree
    if order == 2:
        return 17 + degree
    return 22 + degree


def listings():
    groups = []
    parts = []
    segments = []
    spot = 0
    for degree in range(7):
        reach = min(degree, 2)
        span = 2 * degree + 1
        first = degree * degree
        for row in range(2 * reach + 1):
            slot = frame_slot(degree, row - reach)
            base = spot + row * span - first
            segments.append((base + first, (-base) % 4))
            for quad in range(first // 4, (first + span - 1) // 4 + 1):
                low = base + max(4 * quad, first)
                high = base + min(4 * quad + 3, first + span - 1)
                for window in (0, 1):
                    start = max(low, window * LANES)
                    end = min(high, window * LANES + LANES - 1)
                    if start <= end:
                        for which in (0, 1):
                            tile = 2 * quad + which
                            if any((e - base) // 2 == tile for e in range(start, end + 1)):
                                parts.append((slot, tile, len(groups), which))
                        groups.append((window, start, end))
        spot += span * (2 * reach + 1)
    return groups, parts, segments


GROUPS, PARTS, SEGMENTS = listings()
LOW_GROUPS = sum(window == 0 for window, _, _ in GROUPS)
ALL_ROWS = BLOCK * len(GROUPS)


def packed_pairs():
    pairs = []
    starts = []
    for first, count in ORDERS:
        starts.append(len(pairs) * LANES)
        for slot in range(first, first + count, 2):
            pairs.append((slot, min(slot + 1, first + count - 1)))
    return pairs, starts


PAIRS, STARTS = packed_pairs()


def message_starts():
    starts = {}
    spot = 0
    for order in SEND_ORDER:
        starts[order] = spot
        spot += ORDERS[order][1] * HALF
    return starts


SENT = message_starts()
SPLIT = (ORDERS[3][1] + 1) // 2 * LANES


def message_place(slot):
    order = max(o for o, (first, _) in enumerate(ORDERS) if first <= slot)
    place = SENT[order] // HALF + slot - ORDERS[order][0]
    return place // 2, place % 2


def each(count, func):
    if count <= 16:
        for index in range(count):
            func(index)
    else:
        lax.fori_loop(0, count, lambda index, carry: (func(index), carry)[1], 0)


def kernel(
    peers,
    slots,
    x_hbm,
    rot_hbm,
    src_hbm,
    cnt_hbm,
    dst_hbm,
    gain_hbm,
    w0_hbm,
    w1_hbm,
    w2_hbm,
    x_ref,
    total,
    sums_ref,
    rot_ref,
    src_ref,
    cnt_ref,
    dst_ref,
    gain_ref,
    w0_raw,
    w2_raw,
    w0,
    w1,
    w2,
    expand,
    rot_scr,
    entries,
    mult,
    xg,
    turned,
    part_scr,
    y_scr,
    msg,
    recv,
    rrot,
    f_scr,
    back,
    sq,
    sq_other,
    wsem,
    esem,
    rot_sem,
    msg_sem,
    qsem,
):
    me = lax.axis_index("dev")
    half = lax.axis_index("rep")
    nodes = x_ref.shape[0]
    flat = x_ref.shape[1]
    blocks = peers * slots // BLOCK
    group = BLOCK // slots
    partner = {"rep": 1 - half}

    def peer(index):
        return index + lax.div(index + peers - me, peers)

    def load(index, src, dst):
        return pltpu.make_async_copy(src, dst, wsem.at[index])

    early = [
        load(0, rot_hbm, rot_ref),
        load(1, src_hbm, src_ref),
        load(2, cnt_hbm, cnt_ref),
        load(3, x_hbm, x_ref),
    ]
    late = [
        load(4, dst_hbm, dst_ref),
        load(5, w0_hbm, w0_raw),
        load(6, w2_hbm, w2_raw),
        load(8, gain_hbm, gain_ref),
    ]
    width = w1_hbm.shape[-1]
    for side in (0, 1):
        for kind in (0, 1):
            cols = slice(kind * width, (kind + 1) * width)
            late.append(load(7, w1_hbm.at[kind, :, side], w1.at[side, :, :, cols]))
    waits = late[:4] + [load(7, w1, w1)]
    for copy in early + late:
        copy.start()
    barrier = pltpu.get_barrier_semaphore()
    pl.semaphore_signal(barrier, inc=1, device_id=partner, device_id_type=MESH)
    each(
        peers - 1,
        lambda o: pl.semaphore_signal(
            barrier, inc=1, device_id={"dev": peer(o)}, device_id_type=MESH
        ),
    )

    def lanes(rows):
        return lax.broadcasted_iota(jnp.int32, (rows, LANES), 1)

    y_scr[...] = jnp.zeros_like(y_scr)
    xg[:, flat:] = jnp.zeros((BLOCK, xg.shape[1] - flat), jnp.float32)
    for window in (0, 1):
        entry = lax.broadcasted_iota(jnp.int32, (LANES, LANES), 0) + window * LANES
        spot = lax.broadcasted_iota(jnp.int32, (LANES, LANES), 1)
        shift = jnp.zeros_like(entry)
        for start, offset in SEGMENTS:
            shift = jnp.where(entry >= start, offset, shift)
        place = lax.rem(entry + shift, 4)
        for side in (0, 1):
            hit = place == lax.div(spot, HALF) + 2 * side
            expand[window, :, side * LANES : (side + 1) * LANES] = jnp.where(
                hit, 1.0, 0.0
            ).astype(jnp.bfloat16)

    def column(rows):
        row = lax.broadcasted_iota(jnp.int32, (BLOCK, group), 0)
        spot = lax.broadcasted_iota(jnp.int32, (BLOCK, group), 1)
        chosen = jnp.zeros((BLOCK, group), jnp.float32)
        for index in range(slots):
            chosen = jnp.where(row == spot * slots + index, rows[index], chosen)
        return jnp.sum(chosen, axis=1, keepdims=True)

    def sources(block):
        count = cnt_ref[block]
        value = src_ref[block]
        return column(
            [
                jnp.where(count > index, value[index : index + 1], -1).astype(jnp.float32)
                for index in range(slots)
            ]
        )

    def targets(block):
        value = dst_ref[block].astype(jnp.float32)
        down = column([value[index : index + 1] for index in range(slots)])
        row = lax.broadcasted_iota(jnp.int32, (BLOCK, BLOCK), 0)
        spot = lax.broadcasted_iota(jnp.int32, (BLOCK, BLOCK), 1)
        return jnp.sum(jnp.where(row == spot, down, 0.0), axis=0, keepdims=True)

    def spread(ref, start, edges):
        for index in range(edges // slots):
            rot_scr[index * slots : (index + 1) * slots, 0:ROT] = ref[start + index].astype(
                jnp.float32
            )
        for number, (window, first, last) in enumerate(GROUPS):
            spots = lanes(edges) + window * LANES
            rows = rot_scr[0:edges, window * LANES : (window + 1) * LANES]
            entries[number * edges : (number + 1) * edges, :] = jnp.where(
                (spots >= first) & (spots <= last), rows, 0.0
            ).astype(jnp.bfloat16)
        cut = LOW_GROUPS * edges
        for window, rows in enumerate((slice(0, cut), slice(cut, len(GROUPS) * edges))):
            mult[rows] = jnp.dot(
                entries[rows], expand[window], preferred_element_type=jnp.float32
            )

    def factor(number, which, edges):
        return mult[number * edges : (number + 1) * edges, which * LANES : (which + 1) * LANES]

    def turn(block):
        low_half = lanes(BLOCK) < HALF
        hot = (
            lax.broadcasted_iota(jnp.int32, (BLOCK, nodes), 1).astype(jnp.float32) == sources(block)
        ).astype(jnp.bfloat16)
        spread(rot_ref, block * group, BLOCK)
        if block is first_block:
            early[3].wait()
        xg[:, 0:flat] = jnp.dot(hot, x_ref[...], preferred_element_type=jnp.float32)
        sums = [None] * FRAME
        for slot, tile, number, which in PARTS:
            part = factor(number, which, BLOCK) * xg[:, tile * LANES : (tile + 1) * LANES]
            sums[slot] = part if sums[slot] is None else sums[slot] + part
        for pair, (one, two) in enumerate(PAIRS):
            kept = jnp.where(low_half, sums[one], sums[two])
            moved = jnp.where(low_half, sums[two], sums[one])
            turned[half, block, :, pair * LANES : (pair + 1) * LANES] = (
                kept + pltpu.roll(moved, HALF, 1)
            ).astype(jnp.bfloat16)

    for copy in early[:3]:
        copy.wait()
    first_block = 0 if blocks <= 16 else None
    if first_block is None:
        early[3].wait()
    each(blocks, turn)

    pl.semaphore_wait(barrier, peers)

    exchange = pltpu.make_async_remote_copy(
        src_ref=turned.at[half],
        dst_ref=turned.at[half],
        send_sem=esem.at[0],
        recv_sem=esem.at[1],
        device_id=partner,
        device_id_type=MESH,
    )
    exchange.start()

    share_of = lax.div(me, peers // 2)

    def transfer(source, target, sems, o):
        to = peer(o)
        return pltpu.make_async_remote_copy(
            src_ref=source.at[to],
            dst_ref=target.at[me],
            send_sem=sems.at[2],
            recv_sem=sems.at[share_of],
            device_id={"dev": to},
            device_id_type=MESH,
        )

    def keep(source, target, sems):
        return pltpu.make_async_copy(source.at[me], target.at[me], sems.at[share_of])

    def arrived(target, sems, part):
        span = target.at[pl.ds(part * (peers // 2), peers // 2)]
        return pltpu.make_async_copy(span, span, sems.at[part])

    def sent(source, sems):
        span = source.at[pl.ds(0, peers - 1)]
        return pltpu.make_async_copy(span, span, sems.at[2])

    each(peers - 1, lambda o: transfer(rot_ref, rrot, rot_sem, o).start())
    keep(rot_ref, rrot, rot_sem).start()

    for copy in waits:
        copy.wait()
    for slot in range(ORDERS[0][1]):
        flipped = w0_raw[:, slot * LANES : (slot + 1) * LANES].T
        for side in (0, 1):
            w0[side, slot * HALF : (slot + 1) * HALF, :] = flipped[side * HALF : (side + 1) * HALF]
    for kind in (0, 1):
        for slot in range(ORDERS[3][1]):
            flipped = w2_raw[kind, :, slot * LANES : (slot + 1) * LANES].T
            for side in (0, 1):
                w2[
                    side,
                    slot * HALF : (slot + 1) * HALF,
                    kind * SPLIT : kind * SPLIT + flipped.shape[1],
                ] = flipped[side * HALF : (side + 1) * HALF]

    def product(side, block):
        def rows(order):
            start = STARTS[order]
            return turned[side, block, :, start : start + ORDERS[order][1] * HALF]

        def dot(lhs, rhs):
            return jnp.dot(lhs, rhs, preferred_element_type=jnp.float32)

        results = [dot(rows(0), w0[side])]
        for plus, ref, gap in ((1, w1, width), (3, w2, SPLIT)):
            pair = jnp.concatenate([rows(plus), rows(plus + 1)], axis=0)
            weights = ref[side]
            if weights.ndim == 3:
                weights = weights.reshape(-1, weights.shape[-1])
            both = dot(pair, weights)
            span = ORDERS[plus][1] * HALF
            results.append(both[:BLOCK, :span] - both[BLOCK:, gap : gap + span])
            results.append(both[:BLOCK, gap : gap + span] + both[BLOCK:, :span])
        return results

    def own(block):
        for order, value in enumerate(product(half, block)):
            start = STARTS[order]
            part_scr[block, :, start : start + value.shape[1]] = value

    def mix(block):
        for order, value in enumerate(product(1 - half, block)):
            start = STARTS[order]
            sent = SENT[order]
            y_scr[:, sent : sent + value.shape[1]] = (
                value + part_scr[block, :, start : start + value.shape[1]]
            )
        for index in range(group):
            msg[block * group + index] = y_scr[index * slots : (index + 1) * slots, :].astype(
                jnp.bfloat16
            )

    each(blocks, own)
    exchange.wait()
    each(blocks, mix)
    each(peers - 1, lambda o: transfer(msg, recv, msg_sem, o).start())
    keep(msg, recv, msg_sem).start()

    def collect(start):
        low_half = lanes(PIECE) < HALF
        for index in range(PIECE // slots):
            f_scr[index * slots : (index + 1) * slots, :] = recv[start + index].astype(jnp.float32)
        doubled = {}
        for slot in range(FRAME):
            tile, side = message_place(slot)
            value = f_scr[:, tile * LANES : (tile + 1) * LANES]
            turned = pltpu.roll(value, HALF, 1)
            doubled[slot] = (
                jnp.where(low_half, value, turned) if side == 0 else jnp.where(low_half, turned, value)
            )
        sums = [None] * TILES
        for slot, tile, number, which in PARTS:
            part = factor(number, which, PIECE) * doubled[slot]
            sums[tile] = part if sums[tile] is None else sums[tile] + part
        first = pl.multiple_of(start * slots, PIECE)
        for tile in range(TILES):
            back[pl.ds(first, PIECE), tile * LANES : (tile + 1) * LANES] = sums[tile].astype(
                jnp.bfloat16
            )

    wide = PIECE // slots
    pieces = peers // 2 // wide
    for part in (0, 1):
        arrived(rrot, rot_sem, part).wait()
        base = part * (peers // 2)
        if pieces == 1:
            spread(rrot, base, PIECE)
            arrived(recv, msg_sem, part).wait()
            collect(base)
        else:
            arrived(recv, msg_sem, part).wait()

            def one(piece, carry):
                spread(rrot, base + piece * wide, PIECE)
                collect(base + piece * wide)
                return carry

            lax.fori_loop(0, pieces, one, 0)

    hot = jnp.concatenate(
        [
            (
                lax.broadcasted_iota(jnp.int32, (nodes, BLOCK), 0).astype(jnp.float32)
                == targets(block)
            ).astype(jnp.bfloat16)
            for block in range(blocks)
        ],
        axis=1,
    )
    partial = None
    for start in range(0, WIDE, 2 * LANES):
        cols = slice(start, min(start + 2 * LANES, WIDE))
        value = jnp.dot(hot, back[:, cols], preferred_element_type=jnp.float32)
        total[:, cols] = value
        for part in range(0, cols.stop - start, LANES):
            square = value[:, part : part + LANES] * value[:, part : part + LANES]
            partial = square if partial is None else partial + square
    sq[...] = partial
    share = pltpu.make_async_remote_copy(
        src_ref=sq,
        dst_ref=sq_other,
        send_sem=qsem.at[0],
        recv_sem=qsem.at[1],
        device_id=partner,
        device_id_type=MESH,
    )
    share.start()
    for start in range(0, flat, LANES):
        cols = slice(start, min(start + LANES, flat))
        total[:, cols] = total[:, cols] * gain_ref[:, cols]
    sent(rot_ref, rot_sem).wait()
    sent(msg, msg_sem).wait()
    share.wait()
    sums_ref[...] = sq[...] + sq_other[...]


def finish(chunks, x_ref, total, sums_ref, out_hbm, out_ref, sems):
    flat = x_ref.shape[1]
    mean_sq = jnp.sum(sums_ref[...], axis=1, keepdims=True) / (2 * flat)
    scale = lax.rsqrt(mean_sq + 1e-06)
    copies = []
    for index, (first, last) in enumerate(chunks):
        for start in range(first, last, LANES):
            cols = slice(start, min(start + LANES, last))
            normed = total[:, cols] * scale
            out_ref[:, cols] = (x_ref[:, cols].astype(jnp.float32) + normed).astype(jnp.bfloat16)
        part = slice(first, last)
        copies.append(
            pltpu.make_async_copy(out_ref.at[:, part], out_hbm.at[:, part], sems.at[index])
        )
        copies[-1].start()
    for copy in copies:
        copy.wait()


def shards(node_features, src_node, dst_node, counts, rotation, w_zero, w_one, w_two, norm_gain):
    nodes, _, flat = node_features.shape
    peers, slots = src_node.shape[1:]
    edges = peers * slots
    blocks = edges // BLOCK
    x = node_features.reshape(nodes, flat)
    group = peers // blocks
    src = src_node.reshape(blocks, group, slots).swapaxes(1, 2)
    dst = dst_node.reshape(blocks, group, slots).swapaxes(1, 2)
    cnt = counts.reshape(blocks, 1, group)
    rot = rotation.reshape(peers, slots, ROT)
    w0 = w_zero.reshape(w_zero.shape[0], -1).T
    w1 = w_one.reshape(2, -1, 2, HALF, w_one.shape[-1])
    w2 = w_two.reshape(2, w_two.shape[1], -1).swapaxes(1, 2)
    vmem = pl.BlockSpec(memory_space=pltpu.VMEM)
    hbm = pl.BlockSpec(memory_space=pltpu.HBM)
    f32, bf16 = jnp.float32, jnp.bfloat16
    dma = pltpu.SemaphoreType.DMA
    operands = (x, rot, src, cnt, dst, norm_gain, w0, w1, w2)
    held, total, sums = pl.pallas_call(
        functools.partial(kernel, peers, slots),
        out_shape=(
            jax.ShapeDtypeStruct((nodes, flat), bf16),
            jax.ShapeDtypeStruct((nodes, WIDE), f32),
            jax.ShapeDtypeStruct((nodes, LANES), f32),
        ),
        in_specs=[hbm] * 9,
        out_specs=(vmem,) * 3,
        scratch_shapes=[
            pltpu.VMEM(rot.shape, bf16),
            pltpu.VMEM(src.shape, jnp.int32),
            pltpu.VMEM(cnt.shape, jnp.int32),
            pltpu.VMEM(dst.shape, jnp.int32),
            pltpu.VMEM(norm_gain.shape, f32),
            pltpu.VMEM(w0.shape, bf16),
            pltpu.VMEM(w2.shape, bf16),
            pltpu.VMEM((2, w0.shape[1] // 2, w0.shape[0]), bf16),
            pltpu.VMEM((2, w1.shape[1], HALF, 2 * w1.shape[-1]), bf16),
            pltpu.VMEM((2, w2.shape[2] // 2, 2 * SPLIT), bf16),
            pltpu.VMEM((2, LANES, 2 * LANES), bf16),
            pltpu.VMEM((BLOCK, 2 * LANES), f32),
            pltpu.VMEM((ALL_ROWS, LANES), bf16),
            pltpu.VMEM((ALL_ROWS, 2 * LANES), f32),
            pltpu.VMEM((BLOCK, WIDE), f32),
            pltpu.VMEM((2, blocks, BLOCK, len(PAIRS) * LANES), bf16),
            pltpu.VMEM((blocks, BLOCK, len(PAIRS) * LANES), f32),
            pltpu.VMEM((BLOCK, MESSAGE), f32),
            pltpu.VMEM((peers, slots, MESSAGE), bf16),
            pltpu.VMEM((peers, slots, MESSAGE), bf16),
            pltpu.VMEM((peers, slots, ROT), bf16),
            pltpu.VMEM((PIECE, MESSAGE), f32),
            pltpu.VMEM((edges, WIDE), bf16),
            pltpu.VMEM((nodes, LANES), f32),
            pltpu.VMEM((nodes, LANES), f32),
            dma((9,)),
            dma((2,)),
            dma((3,)),
            dma((3,)),
            dma((2,)),
        ],
        compiler_params=pltpu.CompilerParams(
            collective_id=0, has_side_effects=True, vmem_limit_bytes=VMEM_LIMIT
        ),
    )(*(pltpu.with_memory_space_constraint(operand, pltpu.HBM) for operand in operands))
    cut = (flat // LANES + 3) // 4 * LANES
    chunks = [(start, min(start + cut, flat)) for start in range(0, flat, cut)]
    out = pl.pallas_call(
        functools.partial(finish, chunks),
        out_shape=jax.ShapeDtypeStruct((nodes, flat), bf16),
        in_specs=[vmem] * 3,
        out_specs=hbm,
        scratch_shapes=[pltpu.VMEM((nodes, flat), bf16), dma((len(chunks),))],
        compiler_params=pltpu.CompilerParams(vmem_limit_bytes=VMEM_LIMIT),
    )(held, total, sums)
    return out.reshape(nodes, 1, flat)


def solution(mesh):
    return jax.shard_map(
        shards,
        mesh=mesh,
        in_specs=(
            P("dev", "rep", None),
            P("dev", None, None),
            P("dev", None, None),
            P("dev", None),
            P("dev", None, None, None),
            P(None, "rep", None),
            P(None, None, "rep", None),
            P(None, None, "rep", None),
            P("rep", None),
        ),
        out_specs=P("dev", "rep", None),
        check_vma=False,
    )
```

```python
import functools

import jax
import jax.numpy as jnp
from jax import lax
from jax.experimental import pallas as pl
from jax.experimental.pallas import tpu as pltpu
from jax.sharding import PartitionSpec as P

LANES = 128
HALF = 64
COEFFS = 49
FRAME = 29
ROT = 235
TILES = (COEFFS + 1) // 2
WIDE = TILES * LANES
MESSAGE = (FRAME + 1) // 2 * LANES
VMEM_LIMIT = 40 * 1024 * 1024
BLOCK = 32
PIECE = 16
MESH = pl.DeviceIdType.MESH
ORDERS = ((0, 7), (7, 6), (13, 6), (19, 5), (24, 5))
SEND_ORDER = (0, 4, 1, 2, 3)


def frame_slot(degree, order):
    if order == 0:
        return degree
    if order == 1:
        return 6 + degree
    if order == -1:
        return 12 + degree
    if order == 2:
        return 17 + degree
    return 22 + degree


def listings():
    groups = []
    alone = []
    parts = []
    segments = []
    spot = 0
    for degree in range(7):
        reach = min(degree, 2)
        span = 2 * degree + 1
        first = degree * degree
        for row in range(2 * reach + 1):
            slot = frame_slot(degree, row - reach)
            base = spot + row * span - first
            segments.append((base + first, (-base) % 4))
            for quad in range(first // 4, (first + span - 1) // 4 + 1):
                low = base + max(4 * quad, first)
                high = base + min(4 * quad + 3, first + span - 1)
                if low == high and (low - base) % 2 == 0:
                    parts.append((slot, 2 * quad, len(alone), None))
                    alone.append(low)
                    continue
                for window in (0, 1):
                    start = max(low, window * LANES)
                    end = min(high, window * LANES + LANES - 1)
                    if start <= end:
                        for which in (0, 1):
                            tile = 2 * quad + which
                            if any((e - base) // 2 == tile for e in range(start, end + 1)):
                                parts.append((slot, tile, len(groups), which))
                        groups.append((window, start, end))
        spot += span * (2 * reach + 1)
    return groups, alone, parts, segments


GROUPS, ALONE, PARTS, SEGMENTS = listings()
LOW_GROUPS = sum(window == 0 for window, _, _ in GROUPS)
ALL_ROWS = BLOCK * len(GROUPS)


def packed_pairs():
    pairs = []
    starts = []
    for first, count in ORDERS:
        starts.append(len(pairs) * LANES)
        for slot in range(first, first + count, 2):
            pairs.append((slot, min(slot + 1, first + count - 1)))
    return pairs, starts


PAIRS, STARTS = packed_pairs()


def message_starts():
    starts = {}
    spot = 0
    for order in SEND_ORDER:
        starts[order] = spot
        spot += ORDERS[order][1] * HALF
    return starts


SENT = message_starts()
SPLIT = (ORDERS[3][1] + 1) // 2 * LANES


def message_place(slot):
    order = max(o for o, (first, _) in enumerate(ORDERS) if first <= slot)
    place = SENT[order] // HALF + slot - ORDERS[order][0]
    return place // 2, place % 2


def each(count, func):
    if count <= 16:
        for index in range(count):
            func(index)
    else:
        lax.fori_loop(0, count, lambda index, carry: (func(index), carry)[1], 0)


def kernel(
    peers,
    slots,
    x_hbm,
    rot_hbm,
    src_hbm,
    cnt_hbm,
    dst_hbm,
    gain_hbm,
    w0_hbm,
    w1_hbm,
    w2_hbm,
    x_ref,
    total,
    sums_ref,
    rot_ref,
    src_ref,
    cnt_ref,
    dst_ref,
    gain_ref,
    w0_raw,
    w2_raw,
    w0,
    w1,
    w2,
    expand,
    rot_scr,
    entries,
    mult,
    single,
    xg,
    turned,
    part_scr,
    y_scr,
    msg,
    recv,
    rrot,
    f_scr,
    back,
    sq,
    sq_other,
    wsem,
    esem,
    rot_sem,
    msg_sem,
    qsem,
):
    me = lax.axis_index("dev")
    half = lax.axis_index("rep")
    nodes = x_ref.shape[0]
    flat = x_ref.shape[1]
    blocks = peers * slots // BLOCK
    group = BLOCK // slots
    partner = {"rep": 1 - half}

    side = lax.div(me, peers // 2)

    def peer(index):
        step, odd = index // 2, index % 2
        mixed = (1 - odd) * step + odd * (peers - 2 - step)
        index = side * index + (1 - side) * mixed
        return index + lax.div(index + peers - me, peers)

    def load(index, src, dst):
        return pltpu.make_async_copy(src, dst, wsem.at[index])

    early = [
        load(0, rot_hbm, rot_ref),
        load(1, src_hbm, src_ref),
        load(2, cnt_hbm, cnt_ref),
        load(3, x_hbm, x_ref),
    ]
    late = []
    width = w1_hbm.shape[-1]
    for part in (0, 1):
        for kind in (0, 1):
            cols = slice(kind * width, (kind + 1) * width)
            late.append(load(7, w1_hbm.at[kind, :, part], w1.at[part, :, :, cols]))
    late += [
        load(5, w0_hbm, w0_raw),
        load(6, w2_hbm, w2_raw),
        load(4, dst_hbm, dst_ref),
        load(8, gain_hbm, gain_ref),
    ]
    for copy in (early[3], *early[:3]):
        copy.start()
    barrier = pltpu.get_barrier_semaphore()
    pl.semaphore_signal(barrier, inc=1, device_id=partner, device_id_type=MESH)
    each(
        peers - 1,
        lambda o: pl.semaphore_signal(
            barrier, inc=1, device_id={"dev": peer(o)}, device_id_type=MESH
        ),
    )

    def lanes(rows):
        return lax.broadcasted_iota(jnp.int32, (rows, LANES), 1)

    y_scr[...] = jnp.zeros_like(y_scr)
    xg[:, flat:] = jnp.zeros((BLOCK, xg.shape[1] - flat), jnp.float32)
    for window in (0, 1):
        entry = lax.broadcasted_iota(jnp.int32, (LANES, LANES), 0) + window * LANES
        spot = lax.broadcasted_iota(jnp.int32, (LANES, LANES), 1)
        shift = jnp.zeros_like(entry)
        for start, offset in SEGMENTS:
            shift = jnp.where(entry >= start, offset, shift)
        place = lax.rem(entry + shift, 4)
        for part in (0, 1):
            hit = place == lax.div(spot, HALF) + 2 * part
            expand[window, :, part * LANES : (part + 1) * LANES] = jnp.where(
                hit, 1.0, 0.0
            ).astype(jnp.bfloat16)

    for copy in late:
        copy.start()

    def column(rows):
        row = lax.broadcasted_iota(jnp.int32, (BLOCK, group), 0)
        spot = lax.broadcasted_iota(jnp.int32, (BLOCK, group), 1)
        chosen = jnp.zeros((BLOCK, group), jnp.float32)
        for index in range(slots):
            chosen = jnp.where(row == spot * slots + index, rows[index], chosen)
        return jnp.sum(chosen, axis=1, keepdims=True)

    def sources(block):
        count = cnt_ref[block]
        value = src_ref[block]
        return column(
            [
                jnp.where(count > index, value[index : index + 1], -1).astype(jnp.float32)
                for index in range(slots)
            ]
        )

    def targets(block):
        value = dst_ref[block].astype(jnp.float32)
        down = column([value[index : index + 1] for index in range(slots)])
        row = lax.broadcasted_iota(jnp.int32, (BLOCK, BLOCK), 0)
        spot = lax.broadcasted_iota(jnp.int32, (BLOCK, BLOCK), 1)
        return jnp.sum(jnp.where(row == spot, down, 0.0), axis=0, keepdims=True)

    def place(ref, start, edges, spot=0):
        base = spot * edges
        for index in range(edges // slots):
            first = base + index * slots
            rot_scr[first : first + slots, 0:ROT] = ref[start + index].astype(jnp.float32)
        for number, (window, first, last) in enumerate(GROUPS):
            spots = lanes(edges) + window * LANES
            rows = rot_scr[base : base + edges, window * LANES : (window + 1) * LANES]
            first_row = (spot * len(GROUPS) + number) * edges
            entries[first_row : first_row + edges, :] = jnp.where(
                (spots >= first) & (spots <= last), rows, 0.0
            ).astype(jnp.bfloat16)

    def spread(edges, spot=0):
        base = spot * edges
        low = base * len(GROUPS)
        cut = low + LOW_GROUPS * edges
        high = low + len(GROUPS) * edges
        for window, span in enumerate((slice(low, cut), slice(cut, high))):
            mult[span] = jnp.dot(
                entries[span], expand[window], preferred_element_type=jnp.float32
            )
        for number, entry in enumerate(ALONE):
            value = rot_scr[base : base + edges, entry : entry + 1]
            value = jnp.broadcast_to(value, (edges, LANES))
            first_row = (spot * len(ALONE) + number) * edges
            single[first_row : first_row + edges, :] = jnp.where(
                lanes(edges) < HALF, value, 0.0
            )

    def factor(number, which, edges, spot=0):
        number += spot * len(ALONE if which is None else GROUPS)
        span = slice(number * edges, (number + 1) * edges)
        if which is None:
            return single[span, :]
        return mult[span, which * LANES : (which + 1) * LANES]

    def turn(block):
        low_half = lanes(BLOCK) < HALF
        hot = (
            lax.broadcasted_iota(jnp.int32, (BLOCK, nodes), 1).astype(jnp.float32) == sources(block)
        ).astype(jnp.bfloat16)
        place(rot_ref, block * group, BLOCK)
        if block is first_block:
            early[3].wait()
        spread(BLOCK)
        xg[:, 0:flat] = jnp.dot(hot, x_ref[...], preferred_element_type=jnp.float32)
        sums = [None] * FRAME
        for slot, tile, number, which in PARTS:
            part = factor(number, which, BLOCK) * xg[:, tile * LANES : (tile + 1) * LANES]
            sums[slot] = part if sums[slot] is None else sums[slot] + part
        for pair, (one, two) in enumerate(PAIRS):
            kept = jnp.where(low_half, sums[one], sums[two])
            moved = jnp.where(low_half, sums[two], sums[one])
            turned[half, block, :, pair * LANES : (pair + 1) * LANES] = (
                kept + pltpu.roll(moved, HALF, 1)
            ).astype(jnp.bfloat16)

    for copy in early[:3]:
        copy.wait()
    first_block = 0 if blocks <= 16 else None
    if first_block is None:
        early[3].wait()
    each(blocks, turn)

    pl.semaphore_wait(barrier, peers)

    exchange = pltpu.make_async_remote_copy(
        src_ref=turned.at[half],
        dst_ref=turned.at[half],
        send_sem=esem.at[0],
        recv_sem=esem.at[1],
        device_id=partner,
        device_id_type=MESH,
    )
    exchange.start()

    def transfer(source, target, sems, o):
        to = peer(o)
        return pltpu.make_async_remote_copy(
            src_ref=source.at[to],
            dst_ref=target.at[me],
            send_sem=sems.at[2],
            recv_sem=sems.at[side],
            device_id={"dev": to},
            device_id_type=MESH,
        )

    def keep(source, target, sems):
        return pltpu.make_async_copy(source.at[me], target.at[me], sems.at[side])

    def arrived(target, sems, part):
        span = target.at[pl.ds(part * (peers // 2), peers // 2)]
        return pltpu.make_async_copy(span, span, sems.at[part])

    def sent(source, sems):
        span = source.at[pl.ds(0, peers - 1)]
        return pltpu.make_async_copy(span, span, sems.at[2])

    each(peers - 1, lambda o: transfer(rot_ref, rrot, rot_sem, o).start())
    keep(rot_ref, rrot, rot_sem).start()

    def rows(part, block, order):
        start = STARTS[order]
        return turned[part, block, :, start : start + ORDERS[order][1] * HALF]

    def product(part, block, order):
        if order == 0:
            lhs = rows(part, block, order)
            return [(0, jnp.dot(lhs, w0[part], preferred_element_type=jnp.float32))]
        lhs = jnp.concatenate(
            [rows(part, block, order), rows(part, block, order + 1)], axis=0
        )
        rhs, gap = (w1[part], width) if order == 1 else (w2[part], SPLIT)
        if rhs.ndim == 3:
            rhs = rhs.reshape(-1, rhs.shape[-1])
        both = jnp.dot(lhs, rhs, preferred_element_type=jnp.float32)
        span = ORDERS[order][1] * HALF
        plus = both[:BLOCK, :span] - both[BLOCK:, gap : gap + span]
        minus = both[:BLOCK, gap : gap + span] + both[BLOCK:, :span]
        return [(order, plus), (order + 1, minus)]

    def own(order):
        def one(block):
            for spot, value in product(half, block, order):
                start = STARTS[spot]
                part_scr[block, :, start : start + value.shape[1]] = value

        return one

    load(7, w1, w1).wait()
    late[4].wait()
    for slot in range(ORDERS[0][1]):
        flipped = w0_raw[:, slot * LANES : (slot + 1) * LANES].T
        for part in (0, 1):
            w0[part, slot * HALF : (slot + 1) * HALF, :] = flipped[part * HALF : (part + 1) * HALF]
    each(blocks, own(1))
    late[5].wait()
    for kind in (0, 1):
        for slot in range(ORDERS[3][1]):
            flipped = w2_raw[kind, :, slot * LANES : (slot + 1) * LANES].T
            for part in (0, 1):
                w2[
                    part,
                    slot * HALF : (slot + 1) * HALF,
                    kind * SPLIT : kind * SPLIT + flipped.shape[1],
                ] = flipped[part * HALF : (part + 1) * HALF]
    each(blocks, own(0))
    each(blocks, own(3))

    def mix(block):
        for order in (0, 1, 3):
            for spot, value in product(1 - half, block, order):
                start = STARTS[spot]
                sent = SENT[spot]
                y_scr[:, sent : sent + value.shape[1]] = (
                    value + part_scr[block, :, start : start + value.shape[1]]
                )
        for index in range(group):
            msg[block * group + index] = y_scr[index * slots : (index + 1) * slots, :].astype(
                jnp.bfloat16
            )

    exchange.wait()
    each(blocks, mix)
    each(peers - 1, lambda o: transfer(msg, recv, msg_sem, o).start())
    keep(msg, recv, msg_sem).start()

    def collect(start, spot=0):
        low_half = lanes(PIECE) < HALF
        for index in range(PIECE // slots):
            f_scr[index * slots : (index + 1) * slots, :] = recv[start + index].astype(jnp.float32)
        doubled = {}
        for slot in range(FRAME):
            tile, side = message_place(slot)
            value = f_scr[:, tile * LANES : (tile + 1) * LANES]
            turned = pltpu.roll(value, HALF, 1)
            doubled[slot] = (
                jnp.where(low_half, value, turned) if side == 0 else jnp.where(low_half, turned, value)
            )
        sums = [None] * TILES
        for slot, tile, number, which in PARTS:
            part = factor(number, which, PIECE, spot) * doubled[slot]
            sums[tile] = part if sums[tile] is None else sums[tile] + part
        first = pl.multiple_of(start * slots, PIECE)
        for tile in range(TILES):
            back[pl.ds(first, PIECE), tile * LANES : (tile + 1) * LANES] = sums[tile].astype(
                jnp.bfloat16
            )

    wide = PIECE // slots
    pieces = peers // 2 // wide
    late[6].wait()
    late[7].wait()
    if pieces == 1:
        for part in (0, 1):
            arrived(rrot, rot_sem, part).wait()
            place(rrot, part * wide, PIECE, part)
            spread(PIECE, part)
        for part in (0, 1):
            arrived(recv, msg_sem, part).wait()
            collect(part * wide, part)
    else:
        for part in (0, 1):
            arrived(rrot, rot_sem, part).wait()
            arrived(recv, msg_sem, part).wait()
            base = part * (peers // 2)

            def one(piece, carry):
                place(rrot, base + piece * wide, PIECE)
                spread(PIECE)
                collect(base + piece * wide)
                return carry

            lax.fori_loop(0, pieces, one, 0)

    hot = jnp.concatenate(
        [
            (
                lax.broadcasted_iota(jnp.int32, (nodes, BLOCK), 0).astype(jnp.float32)
                == targets(block)
            ).astype(jnp.bfloat16)
            for block in range(blocks)
        ],
        axis=1,
    )
    partial = None
    for start in range(0, WIDE, 2 * LANES):
        cols = slice(start, min(start + 2 * LANES, WIDE))
        value = jnp.dot(hot, back[:, cols], preferred_element_type=jnp.float32)
        total[:, cols] = value
        for part in range(0, cols.stop - start, LANES):
            square = value[:, part : part + LANES] * value[:, part : part + LANES]
            partial = square if partial is None else partial + square
    sq[...] = partial
    share = pltpu.make_async_remote_copy(
        src_ref=sq,
        dst_ref=sq_other,
        send_sem=qsem.at[0],
        recv_sem=qsem.at[1],
        device_id=partner,
        device_id_type=MESH,
    )
    share.start()
    for start in range(0, flat, LANES):
        cols = slice(start, min(start + LANES, flat))
        total[:, cols] = total[:, cols] * gain_ref[:, cols]
    sent(rot_ref, rot_sem).wait()
    sent(msg, msg_sem).wait()
    share.wait()
    sums_ref[...] = sq[...] + sq_other[...]


def finish(chunks, x_ref, total, sums_ref, out_hbm, out_ref, sems):
    flat = x_ref.shape[1]
    mean_sq = jnp.sum(sums_ref[...], axis=1, keepdims=True) / (2 * flat)
    scale = lax.rsqrt(mean_sq + 1e-06)
    copies = []
    for index, (first, last) in enumerate(chunks):
        for start in range(first, last, LANES):
            cols = slice(start, min(start + LANES, last))
            normed = total[:, cols] * scale
            out_ref[:, cols] = (x_ref[:, cols].astype(jnp.float32) + normed).astype(jnp.bfloat16)
        part = slice(first, last)
        copies.append(
            pltpu.make_async_copy(out_ref.at[:, part], out_hbm.at[:, part], sems.at[index])
        )
        copies[-1].start()
    for copy in copies:
        copy.wait()


def shards(node_features, src_node, dst_node, counts, rotation, w_zero, w_one, w_two, norm_gain):
    nodes, _, flat = node_features.shape
    peers, slots = src_node.shape[1:]
    edges = peers * slots
    blocks = edges // BLOCK
    x = node_features.reshape(nodes, flat)
    group = peers // blocks
    src = src_node.reshape(blocks, group, slots).swapaxes(1, 2)
    dst = dst_node.reshape(blocks, group, slots).swapaxes(1, 2)
    cnt = counts.reshape(blocks, 1, group)
    rot = rotation.reshape(peers, slots, ROT)
    w0 = w_zero.reshape(w_zero.shape[0], -1).T
    w1 = w_one.reshape(2, -1, 2, HALF, w_one.shape[-1])
    w2 = w_two.reshape(2, w_two.shape[1], -1).swapaxes(1, 2)
    vmem = pl.BlockSpec(memory_space=pltpu.VMEM)
    hbm = pl.BlockSpec(memory_space=pltpu.HBM)
    f32, bf16 = jnp.float32, jnp.bfloat16
    dma = pltpu.SemaphoreType.DMA
    operands = (x, rot, src, cnt, dst, norm_gain, w0, w1, w2)
    held, total, sums = pl.pallas_call(
        functools.partial(kernel, peers, slots),
        out_shape=(
            jax.ShapeDtypeStruct((nodes, flat), bf16),
            jax.ShapeDtypeStruct((nodes, WIDE), f32),
            jax.ShapeDtypeStruct((nodes, LANES), f32),
        ),
        in_specs=[hbm] * 9,
        out_specs=(vmem,) * 3,
        scratch_shapes=[
            pltpu.VMEM(rot.shape, bf16),
            pltpu.VMEM(src.shape, jnp.int32),
            pltpu.VMEM(cnt.shape, jnp.int32),
            pltpu.VMEM(dst.shape, jnp.int32),
            pltpu.VMEM(norm_gain.shape, f32),
            pltpu.VMEM(w0.shape, bf16),
            pltpu.VMEM(w2.shape, bf16),
            pltpu.VMEM((2, w0.shape[1] // 2, w0.shape[0]), bf16),
            pltpu.VMEM((2, w1.shape[1], HALF, 2 * w1.shape[-1]), bf16),
            pltpu.VMEM((2, w2.shape[2] // 2, 2 * SPLIT), bf16),
            pltpu.VMEM((2, LANES, 2 * LANES), bf16),
            pltpu.VMEM((BLOCK, 2 * LANES), f32),
            pltpu.VMEM((ALL_ROWS, LANES), bf16),
            pltpu.VMEM((ALL_ROWS, 2 * LANES), f32),
            pltpu.VMEM((BLOCK * len(ALONE), LANES), f32),
            pltpu.VMEM((BLOCK, WIDE), f32),
            pltpu.VMEM((2, blocks, BLOCK, len(PAIRS) * LANES), bf16),
            pltpu.VMEM((blocks, BLOCK, len(PAIRS) * LANES), f32),
            pltpu.VMEM((BLOCK, MESSAGE), f32),
            pltpu.VMEM((peers, slots, MESSAGE), bf16),
            pltpu.VMEM((peers, slots, MESSAGE), bf16),
            pltpu.VMEM((peers, slots, ROT), bf16),
            pltpu.VMEM((PIECE, MESSAGE), f32),
            pltpu.VMEM((edges, WIDE), bf16),
            pltpu.VMEM((nodes, LANES), f32),
            pltpu.VMEM((nodes, LANES), f32),
            dma((9,)),
            dma((2,)),
            dma((3,)),
            dma((3,)),
            dma((2,)),
        ],
        compiler_params=pltpu.CompilerParams(
            collective_id=0, has_side_effects=True, vmem_limit_bytes=VMEM_LIMIT
        ),
    )(*(pltpu.with_memory_space_constraint(operand, pltpu.HBM) for operand in operands))
    cut = (flat // LANES + 3) // 4 * LANES
    chunks = [(start, min(start + cut, flat)) for start in range(0, flat, cut)]
    out = pl.pallas_call(
        functools.partial(finish, chunks),
        out_shape=jax.ShapeDtypeStruct((nodes, flat), bf16),
        in_specs=[vmem] * 3,
        out_specs=hbm,
        scratch_shapes=[pltpu.VMEM((nodes, flat), bf16), dma((len(chunks),))],
        compiler_params=pltpu.CompilerParams(vmem_limit_bytes=VMEM_LIMIT),
    )(held, total, sums)
    return out.reshape(nodes, 1, flat)


def solution(mesh):
    return jax.shard_map(
        shards,
        mesh=mesh,
        in_specs=(
            P("dev", "rep", None),
            P("dev", None, None),
            P("dev", None, None),
            P("dev", None),
            P("dev", None, None, None),
            P(None, "rep", None),
            P(None, None, "rep", None),
            P(None, None, "rep", None),
            P("rep", None),
        ),
        out_specs=P("dev", "rep", None),
        check_vma=False,
    )
```

```python
import functools

import jax
import jax.numpy as jnp
from jax import lax
from jax.experimental import pallas as pl
from jax.experimental.pallas import tpu as pltpu
from jax.sharding import PartitionSpec as P

LANES = 128
HALF = 64
COEFFS = 49
FRAME = 29
ROT = 235
TILES = (COEFFS + 1) // 2
WIDE = TILES * LANES
MESSAGE = (FRAME + 1) // 2 * LANES
VMEM_LIMIT = 40 * 1024 * 1024
BLOCK = 32
PIECE = 16
MESH = pl.DeviceIdType.MESH
ORDERS = ((0, 7), (7, 6), (13, 6), (19, 5), (24, 5))
SEND_ORDER = (0, 4, 1, 2, 3)


def frame_slot(degree, order):
    if order == 0:
        return degree
    if order == 1:
        return 6 + degree
    if order == -1:
        return 12 + degree
    if order == 2:
        return 17 + degree
    return 22 + degree


def listings():
    groups = []
    alone = []
    parts = []
    segments = []
    spot = 0
    for degree in range(7):
        reach = min(degree, 2)
        span = 2 * degree + 1
        first = degree * degree
        for row in range(2 * reach + 1):
            slot = frame_slot(degree, row - reach)
            base = spot + row * span - first
            segments.append((base + first, (-base) % 4))
            for quad in range(first // 4, (first + span - 1) // 4 + 1):
                low = base + max(4 * quad, first)
                high = base + min(4 * quad + 3, first + span - 1)
                if low == high and (low - base) % 2 == 0:
                    parts.append((slot, 2 * quad, len(alone), None))
                    alone.append(low)
                    continue
                for window in (0, 1):
                    start = max(low, window * LANES)
                    end = min(high, window * LANES + LANES - 1)
                    if start <= end:
                        for which in (0, 1):
                            tile = 2 * quad + which
                            if any((e - base) // 2 == tile for e in range(start, end + 1)):
                                parts.append((slot, tile, len(groups), which))
                        groups.append((window, start, end))
        spot += span * (2 * reach + 1)
    return groups, alone, parts, segments


GROUPS, ALONE, PARTS, SEGMENTS = listings()
LOW_GROUPS = sum(window == 0 for window, _, _ in GROUPS)
ALL_ROWS = BLOCK * len(GROUPS)


def packed_pairs():
    pairs = []
    starts = []
    for first, count in ORDERS:
        starts.append(len(pairs) * LANES)
        for slot in range(first, first + count, 2):
            pairs.append((slot, min(slot + 1, first + count - 1)))
    return pairs, starts


PAIRS, STARTS = packed_pairs()


def message_starts():
    starts = {}
    spot = 0
    for order in SEND_ORDER:
        starts[order] = spot
        spot += ORDERS[order][1] * HALF
    return starts


SENT = message_starts()
SPLIT = (ORDERS[3][1] + 1) // 2 * LANES


def message_place(slot):
    order = max(o for o, (first, _) in enumerate(ORDERS) if first <= slot)
    place = SENT[order] // HALF + slot - ORDERS[order][0]
    return place // 2, place % 2


def each(count, func):
    if count <= 16:
        for index in range(count):
            func(index)
    else:
        lax.fori_loop(0, count, lambda index, carry: (func(index), carry)[1], 0)


def kernel(
    peers,
    slots,
    x_hbm,
    rot_hbm,
    src_hbm,
    cnt_hbm,
    dst_hbm,
    gain_hbm,
    w0_hbm,
    w1_hbm,
    w2_hbm,
    x_ref,
    total,
    sums_ref,
    rot_ref,
    src_ref,
    cnt_ref,
    dst_ref,
    gain_ref,
    w0_raw,
    w2_raw,
    w0,
    w1,
    w2,
    expand,
    rot_scr,
    entries,
    mult,
    single,
    xg,
    turned,
    part_scr,
    y_scr,
    msg,
    recv,
    rrot,
    f_scr,
    back,
    sq,
    sq_other,
    wsem,
    esem,
    rot_sem,
    msg_sem,
    qsem,
):
    me = lax.axis_index("dev")
    half = lax.axis_index("rep")
    nodes = x_ref.shape[0]
    flat = x_ref.shape[1]
    blocks = peers * slots // BLOCK
    group = BLOCK // slots
    partner = {"rep": 1 - half}

    side = lax.div(me, peers // 2)

    def peer(index):
        index = lax.rem(index + half * (peers - 1 - peers // 2), peers - 1)
        step, odd = index // 2, index % 2
        mixed = (1 - odd) * step + odd * (peers - 2 - step)
        index = side * index + (1 - side) * mixed
        return index + lax.div(index + peers - me, peers)

    def load(index, src, dst):
        return pltpu.make_async_copy(src, dst, wsem.at[index])

    early = [
        load(0, rot_hbm, rot_ref),
        load(1, src_hbm, src_ref),
        load(2, cnt_hbm, cnt_ref),
        load(3, x_hbm, x_ref),
    ]
    late = []
    width = w1_hbm.shape[-1]
    for part in (0, 1):
        for kind in (0, 1):
            cols = slice(kind * width, (kind + 1) * width)
            late.append(load(7, w1_hbm.at[kind, :, part], w1.at[part, :, :, cols]))
    late += [
        load(5, w0_hbm, w0_raw),
        load(6, w2_hbm, w2_raw),
        load(4, dst_hbm, dst_ref),
        load(8, gain_hbm, gain_ref),
    ]
    for copy in (early[3], *early[:3]):
        copy.start()
    barrier = pltpu.get_barrier_semaphore()
    pl.semaphore_signal(barrier, inc=1, device_id=partner, device_id_type=MESH)
    each(
        peers - 1,
        lambda o: pl.semaphore_signal(
            barrier, inc=1, device_id={"dev": peer(o)}, device_id_type=MESH
        ),
    )

    def lanes(rows):
        return lax.broadcasted_iota(jnp.int32, (rows, LANES), 1)

    y_scr[...] = jnp.zeros_like(y_scr)
    xg[:, flat:] = jnp.zeros((BLOCK, xg.shape[1] - flat), jnp.float32)
    for window in (0, 1):
        entry = lax.broadcasted_iota(jnp.int32, (LANES, LANES), 0) + window * LANES
        spot = lax.broadcasted_iota(jnp.int32, (LANES, LANES), 1)
        shift = jnp.zeros_like(entry)
        for start, offset in SEGMENTS:
            shift = jnp.where(entry >= start, offset, shift)
        place = lax.rem(entry + shift, 4)
        for part in (0, 1):
            hit = place == lax.div(spot, HALF) + 2 * part
            expand[window, :, part * LANES : (part + 1) * LANES] = jnp.where(
                hit, 1.0, 0.0
            ).astype(jnp.bfloat16)

    for copy in late:
        copy.start()

    def column(rows):
        row = lax.broadcasted_iota(jnp.int32, (BLOCK, group), 0)
        spot = lax.broadcasted_iota(jnp.int32, (BLOCK, group), 1)
        chosen = jnp.zeros((BLOCK, group), jnp.float32)
        for index in range(slots):
            chosen = jnp.where(row == spot * slots + index, rows[index], chosen)
        return jnp.sum(chosen, axis=1, keepdims=True)

    def sources(block):
        count = cnt_ref[block]
        value = src_ref[block]
        return column(
            [
                jnp.where(count > index, value[index : index + 1], -1).astype(jnp.float32)
                for index in range(slots)
            ]
        )

    def targets(block):
        value = dst_ref[block].astype(jnp.float32)
        down = column([value[index : index + 1] for index in range(slots)])
        row = lax.broadcasted_iota(jnp.int32, (BLOCK, BLOCK), 0)
        spot = lax.broadcasted_iota(jnp.int32, (BLOCK, BLOCK), 1)
        return jnp.sum(jnp.where(row == spot, down, 0.0), axis=0, keepdims=True)

    def place(ref, start, edges, spot=0):
        base = spot * edges
        for index in range(edges // slots):
            first = base + index * slots
            rot_scr[first : first + slots, 0:ROT] = ref[start + index].astype(jnp.float32)
        for number, (window, first, last) in enumerate(GROUPS):
            spots = lanes(edges) + window * LANES
            rows = rot_scr[base : base + edges, window * LANES : (window + 1) * LANES]
            first_row = (spot * len(GROUPS) + number) * edges
            entries[first_row : first_row + edges, :] = jnp.where(
                (spots >= first) & (spots <= last), rows, 0.0
            ).astype(jnp.bfloat16)

    def spread(edges, spot=0):
        base = spot * edges
        low = base * len(GROUPS)
        cut = low + LOW_GROUPS * edges
        high = low + len(GROUPS) * edges
        for window, span in enumerate((slice(low, cut), slice(cut, high))):
            mult[span] = jnp.dot(
                entries[span], expand[window], preferred_element_type=jnp.float32
            )
        for number, entry in enumerate(ALONE):
            value = rot_scr[base : base + edges, entry : entry + 1]
            value = jnp.broadcast_to(value, (edges, LANES))
            first_row = (spot * len(ALONE) + number) * edges
            single[first_row : first_row + edges, :] = jnp.where(
                lanes(edges) < HALF, value, 0.0
            )

    def factor(number, which, edges, spot=0):
        number += spot * len(ALONE if which is None else GROUPS)
        span = slice(number * edges, (number + 1) * edges)
        if which is None:
            return single[span, :]
        return mult[span, which * LANES : (which + 1) * LANES]

    def turn(block):
        low_half = lanes(BLOCK) < HALF
        hot = (
            lax.broadcasted_iota(jnp.int32, (BLOCK, nodes), 1).astype(jnp.float32) == sources(block)
        ).astype(jnp.bfloat16)
        place(rot_ref, block * group, BLOCK)
        if block is first_block:
            early[3].wait()
        spread(BLOCK)
        xg[:, 0:flat] = jnp.dot(hot, x_ref[...], preferred_element_type=jnp.float32)
        sums = [None] * FRAME
        for slot, tile, number, which in PARTS:
            part = factor(number, which, BLOCK) * xg[:, tile * LANES : (tile + 1) * LANES]
            sums[slot] = part if sums[slot] is None else sums[slot] + part
        for pair, (one, two) in enumerate(PAIRS):
            kept = jnp.where(low_half, sums[one], sums[two])
            moved = jnp.where(low_half, sums[two], sums[one])
            turned[half, block, :, pair * LANES : (pair + 1) * LANES] = (
                kept + pltpu.roll(moved, HALF, 1)
            ).astype(jnp.bfloat16)

    for copy in early[:3]:
        copy.wait()
    first_block = 0 if blocks <= 16 else None
    if first_block is None:
        early[3].wait()
    each(blocks, turn)

    pl.semaphore_wait(barrier, peers)

    exchange = pltpu.make_async_remote_copy(
        src_ref=turned.at[half],
        dst_ref=turned.at[half],
        send_sem=esem.at[0],
        recv_sem=esem.at[1],
        device_id=partner,
        device_id_type=MESH,
    )
    exchange.start()

    def transfer(source, target, sems, o):
        to = peer(o)
        return pltpu.make_async_remote_copy(
            src_ref=source.at[to],
            dst_ref=target.at[me],
            send_sem=sems.at[2],
            recv_sem=sems.at[side],
            device_id={"dev": to},
            device_id_type=MESH,
        )

    def keep(source, target, sems):
        return pltpu.make_async_copy(source.at[me], target.at[me], sems.at[side])

    def arrived(target, sems, part):
        span = target.at[pl.ds(part * (peers // 2), peers // 2)]
        return pltpu.make_async_copy(span, span, sems.at[part])

    def sent(source, sems):
        span = source.at[pl.ds(0, peers - 1)]
        return pltpu.make_async_copy(span, span, sems.at[2])

    each(peers - 1, lambda o: transfer(rot_ref, rrot, rot_sem, o).start())
    keep(rot_ref, rrot, rot_sem).start()

    def rows(part, block, order):
        start = STARTS[order]
        return turned[part, block, :, start : start + ORDERS[order][1] * HALF]

    def product(part, block, order):
        if order == 0:
            lhs = rows(part, block, order)
            return [(0, jnp.dot(lhs, w0[part], preferred_element_type=jnp.float32))]
        lhs = jnp.concatenate(
            [rows(part, block, order), rows(part, block, order + 1)], axis=0
        )
        rhs, gap = (w1[part], width) if order == 1 else (w2[part], SPLIT)
        if rhs.ndim == 3:
            rhs = rhs.reshape(-1, rhs.shape[-1])
        both = jnp.dot(lhs, rhs, preferred_element_type=jnp.float32)
        span = ORDERS[order][1] * HALF
        plus = both[:BLOCK, :span] - both[BLOCK:, gap : gap + span]
        minus = both[:BLOCK, gap : gap + span] + both[BLOCK:, :span]
        return [(order, plus), (order + 1, minus)]

    def own(order):
        def one(block):
            for spot, value in product(half, block, order):
                start = STARTS[spot]
                part_scr[block, :, start : start + value.shape[1]] = value

        return one

    load(7, w1, w1).wait()
    late[4].wait()
    for slot in range(ORDERS[0][1]):
        flipped = w0_raw[:, slot * LANES : (slot + 1) * LANES].T
        for part in (0, 1):
            w0[part, slot * HALF : (slot + 1) * HALF, :] = flipped[part * HALF : (part + 1) * HALF]
    each(blocks, own(1))
    late[5].wait()
    for kind in (0, 1):
        for slot in range(ORDERS[3][1]):
            flipped = w2_raw[kind, :, slot * LANES : (slot + 1) * LANES].T
            for part in (0, 1):
                w2[
                    part,
                    slot * HALF : (slot + 1) * HALF,
                    kind * SPLIT : kind * SPLIT + flipped.shape[1],
                ] = flipped[part * HALF : (part + 1) * HALF]
    each(blocks, own(0))
    each(blocks, own(3))

    def mix(block):
        values = []
        for order in (3, 1, 0):
            values += product(1 - half, block, order)
        for spot, value in values:
            start = STARTS[spot]
            sent = SENT[spot]
            y_scr[:, sent : sent + value.shape[1]] = (
                value + part_scr[block, :, start : start + value.shape[1]]
            )
        for index in range(group):
            msg[block * group + index] = y_scr[index * slots : (index + 1) * slots, :].astype(
                jnp.bfloat16
            )

    exchange.wait_recv()
    each(blocks, mix)
    each(peers - 1, lambda o: transfer(msg, recv, msg_sem, o).start())
    keep(msg, recv, msg_sem).start()

    def collect(start, spot=0):
        low_half = lanes(PIECE) < HALF
        for index in range(PIECE // slots):
            f_scr[index * slots : (index + 1) * slots, :] = recv[start + index].astype(jnp.float32)
        doubled = {}
        for slot in range(FRAME):
            tile, side = message_place(slot)
            value = f_scr[:, tile * LANES : (tile + 1) * LANES]
            turned = pltpu.roll(value, HALF, 1)
            doubled[slot] = (
                jnp.where(low_half, value, turned) if side == 0 else jnp.where(low_half, turned, value)
            )
        sums = [None] * TILES
        for slot, tile, number, which in PARTS:
            part = factor(number, which, PIECE, spot) * doubled[slot]
            sums[tile] = part if sums[tile] is None else sums[tile] + part
        first = pl.multiple_of(start * slots, PIECE)
        for tile in range(TILES):
            back[pl.ds(first, PIECE), tile * LANES : (tile + 1) * LANES] = sums[tile].astype(
                jnp.bfloat16
            )

    wide = PIECE // slots
    pieces = peers // 2 // wide
    late[6].wait()
    late[7].wait()
    if pieces == 1:
        for part in (0, 1):
            arrived(rrot, rot_sem, part).wait()
            place(rrot, part * wide, PIECE, part)
            spread(PIECE, part)
        for part in (0, 1):
            arrived(recv, msg_sem, part).wait()
            collect(part * wide, part)
    else:
        for part in (0, 1):
            arrived(rrot, rot_sem, part).wait()
            arrived(recv, msg_sem, part).wait()
            base = part * (peers // 2)

            def one(piece, carry):
                place(rrot, base + piece * wide, PIECE)
                spread(PIECE)
                collect(base + piece * wide)
                return carry

            lax.fori_loop(0, pieces, one, 0)

    hot = jnp.concatenate(
        [
            (
                lax.broadcasted_iota(jnp.int32, (nodes, BLOCK), 0).astype(jnp.float32)
                == targets(block)
            ).astype(jnp.bfloat16)
            for block in range(blocks)
        ],
        axis=1,
    )
    partial = None
    for start in range(0, WIDE, 2 * LANES):
        cols = slice(start, min(start + 2 * LANES, WIDE))
        value = jnp.dot(hot, back[:, cols], preferred_element_type=jnp.float32)
        total[:, cols] = value
        for part in range(0, cols.stop - start, LANES):
            square = value[:, part : part + LANES] * value[:, part : part + LANES]
            partial = square if partial is None else partial + square
    sq[...] = partial
    share = pltpu.make_async_remote_copy(
        src_ref=sq,
        dst_ref=sq_other,
        send_sem=qsem.at[0],
        recv_sem=qsem.at[1],
        device_id=partner,
        device_id_type=MESH,
    )
    share.start()
    for start in range(0, flat, LANES):
        cols = slice(start, min(start + LANES, flat))
        total[:, cols] = total[:, cols] * gain_ref[:, cols]
    exchange.wait_send()
    sent(rot_ref, rot_sem).wait()
    sent(msg, msg_sem).wait()
    share.wait()
    sums_ref[...] = sq[...] + sq_other[...]


def finish(chunks, x_ref, total, sums_ref, out_hbm, out_ref, sems):
    flat = x_ref.shape[1]
    mean_sq = jnp.sum(sums_ref[...], axis=1, keepdims=True) / (2 * flat)
    scale = lax.rsqrt(mean_sq + 1e-06)
    copies = []
    for index, (first, last) in enumerate(chunks):
        for start in range(first, last, LANES):
            cols = slice(start, min(start + LANES, last))
            normed = total[:, cols] * scale
            out_ref[:, cols] = (x_ref[:, cols].astype(jnp.float32) + normed).astype(jnp.bfloat16)
        part = slice(first, last)
        copies.append(
            pltpu.make_async_copy(out_ref.at[:, part], out_hbm.at[:, part], sems.at[index])
        )
        copies[-1].start()
    for copy in copies:
        copy.wait()


def shards(node_features, src_node, dst_node, counts, rotation, w_zero, w_one, w_two, norm_gain):
    nodes, _, flat = node_features.shape
    peers, slots = src_node.shape[1:]
    edges = peers * slots
    blocks = edges // BLOCK
    x = node_features.reshape(nodes, flat)
    group = peers // blocks
    src = src_node.reshape(blocks, group, slots).swapaxes(1, 2)
    dst = dst_node.reshape(blocks, group, slots).swapaxes(1, 2)
    cnt = counts.reshape(blocks, 1, group)
    rot = rotation.reshape(peers, slots, ROT)
    w0 = w_zero.reshape(w_zero.shape[0], -1).T
    w1 = w_one.reshape(2, -1, 2, HALF, w_one.shape[-1])
    w2 = w_two.reshape(2, w_two.shape[1], -1).swapaxes(1, 2)
    vmem = pl.BlockSpec(memory_space=pltpu.VMEM)
    hbm = pl.BlockSpec(memory_space=pltpu.HBM)
    f32, bf16 = jnp.float32, jnp.bfloat16
    dma = pltpu.SemaphoreType.DMA
    operands = (x, rot, src, cnt, dst, norm_gain, w0, w1, w2)
    held, total, sums = pl.pallas_call(
        functools.partial(kernel, peers, slots),
        out_shape=(
            jax.ShapeDtypeStruct((nodes, flat), bf16),
            jax.ShapeDtypeStruct((nodes, WIDE), f32),
            jax.ShapeDtypeStruct((nodes, LANES), f32),
        ),
        in_specs=[hbm] * 9,
        out_specs=(vmem,) * 3,
        scratch_shapes=[
            pltpu.VMEM(rot.shape, bf16),
            pltpu.VMEM(src.shape, jnp.int32),
            pltpu.VMEM(cnt.shape, jnp.int32),
            pltpu.VMEM(dst.shape, jnp.int32),
            pltpu.VMEM(norm_gain.shape, f32),
            pltpu.VMEM(w0.shape, bf16),
            pltpu.VMEM(w2.shape, bf16),
            pltpu.VMEM((2, w0.shape[1] // 2, w0.shape[0]), bf16),
            pltpu.VMEM((2, w1.shape[1], HALF, 2 * w1.shape[-1]), bf16),
            pltpu.VMEM((2, w2.shape[2] // 2, 2 * SPLIT), bf16),
            pltpu.VMEM((2, LANES, 2 * LANES), bf16),
            pltpu.VMEM((BLOCK, 2 * LANES), f32),
            pltpu.VMEM((ALL_ROWS, LANES), bf16),
            pltpu.VMEM((ALL_ROWS, 2 * LANES), f32),
            pltpu.VMEM((BLOCK * len(ALONE), LANES), f32),
            pltpu.VMEM((BLOCK, WIDE), f32),
            pltpu.VMEM((2, blocks, BLOCK, len(PAIRS) * LANES), bf16),
            pltpu.VMEM((blocks, BLOCK, len(PAIRS) * LANES), f32),
            pltpu.VMEM((BLOCK, MESSAGE), f32),
            pltpu.VMEM((peers, slots, MESSAGE), bf16),
            pltpu.VMEM((peers, slots, MESSAGE), bf16),
            pltpu.VMEM((peers, slots, ROT), bf16),
            pltpu.VMEM((PIECE, MESSAGE), f32),
            pltpu.VMEM((edges, WIDE), bf16),
            pltpu.VMEM((nodes, LANES), f32),
            pltpu.VMEM((nodes, LANES), f32),
            dma((9,)),
            dma((2,)),
            dma((3,)),
            dma((3,)),
            dma((2,)),
        ],
        compiler_params=pltpu.CompilerParams(
            collective_id=0, has_side_effects=True, vmem_limit_bytes=VMEM_LIMIT
        ),
    )(*(pltpu.with_memory_space_constraint(operand, pltpu.HBM) for operand in operands))
    cut = (flat // LANES + 3) // 4 * LANES
    chunks = [(start, min(start + cut, flat)) for start in range(0, flat, cut)]
    out = pl.pallas_call(
        functools.partial(finish, chunks),
        out_shape=jax.ShapeDtypeStruct((nodes, flat), bf16),
        in_specs=[vmem] * 3,
        out_specs=hbm,
        scratch_shapes=[pltpu.VMEM((nodes, flat), bf16), dma((len(chunks),))],
        compiler_params=pltpu.CompilerParams(vmem_limit_bytes=VMEM_LIMIT),
    )(held, total, sums)
    return out.reshape(nodes, 1, flat)


def solution(mesh):
    return jax.shard_map(
        shards,
        mesh=mesh,
        in_specs=(
            P("dev", "rep", None),
            P("dev", None, None),
            P("dev", None, None),
            P("dev", None),
            P("dev", None, None, None),
            P(None, "rep", None),
            P(None, None, "rep", None),
            P(None, None, "rep", None),
            P("rep", None),
        ),
        out_specs=P("dev", "rep", None),
        check_vma=False,
    )
```

```python
import functools

import jax
import jax.numpy as jnp
from jax import lax
from jax.experimental import pallas as pl
from jax.experimental.pallas import tpu as pltpu
from jax.sharding import PartitionSpec as P

LANES = 128
HALF = 64
COEFFS = 49
FRAME = 29
ROT = 235
TILES = (COEFFS + 1) // 2
WIDE = TILES * LANES
MESSAGE = (FRAME + 1) // 2 * LANES
VMEM_LIMIT = 40 * 1024 * 1024
BLOCK = 32
PIECE = 16
MESH = pl.DeviceIdType.MESH
ORDERS = ((0, 7), (7, 6), (13, 6), (19, 5), (24, 5))
SEND_ORDER = (0, 4, 1, 2, 3)


def frame_slot(degree, order):
    if order == 0:
        return degree
    if order == 1:
        return 6 + degree
    if order == -1:
        return 12 + degree
    if order == 2:
        return 17 + degree
    return 22 + degree


def listings():
    groups = []
    alone = []
    parts = []
    segments = []
    spot = 0
    for degree in range(7):
        reach = min(degree, 2)
        span = 2 * degree + 1
        first = degree * degree
        for row in range(2 * reach + 1):
            slot = frame_slot(degree, row - reach)
            base = spot + row * span - first
            segments.append((base + first, (-base) % 4))
            for quad in range(first // 4, (first + span - 1) // 4 + 1):
                low = base + max(4 * quad, first)
                high = base + min(4 * quad + 3, first + span - 1)
                if low == high and (low - base) % 2 == 0:
                    parts.append((slot, 2 * quad, len(alone), None))
                    alone.append(low)
                    continue
                for window in (0, 1):
                    start = max(low, window * LANES)
                    end = min(high, window * LANES + LANES - 1)
                    if start <= end:
                        for which in (0, 1):
                            tile = 2 * quad + which
                            if any((e - base) // 2 == tile for e in range(start, end + 1)):
                                parts.append((slot, tile, len(groups), which))
                        groups.append((window, start, end))
        spot += span * (2 * reach + 1)
    return groups, alone, parts, segments


GROUPS, ALONE, PARTS, SEGMENTS = listings()
LOW_GROUPS = sum(window == 0 for window, _, _ in GROUPS)
ALL_ROWS = BLOCK * len(GROUPS)


def packed_pairs():
    pairs = []
    starts = []
    for first, count in ORDERS:
        starts.append(len(pairs) * LANES)
        for slot in range(first, first + count, 2):
            pairs.append((slot, min(slot + 1, first + count - 1)))
    return pairs, starts


PAIRS, STARTS = packed_pairs()


def message_starts():
    starts = {}
    spot = 0
    for order in SEND_ORDER:
        starts[order] = spot
        spot += ORDERS[order][1] * HALF
    return starts


SENT = message_starts()
SPLIT = (ORDERS[3][1] + 1) // 2 * LANES


def message_place(slot):
    order = max(o for o, (first, _) in enumerate(ORDERS) if first <= slot)
    place = SENT[order] // HALF + slot - ORDERS[order][0]
    return place // 2, place % 2


def each(count, func):
    if count <= 16:
        for index in range(count):
            func(index)
    else:
        lax.fori_loop(0, count, lambda index, carry: (func(index), carry)[1], 0)


def kernel(
    peers,
    slots,
    x_hbm,
    rot_hbm,
    src_hbm,
    cnt_hbm,
    dst_hbm,
    gain_hbm,
    w0_hbm,
    w1_hbm,
    w2_hbm,
    x_ref,
    total,
    sums_ref,
    rot_ref,
    src_ref,
    cnt_ref,
    dst_ref,
    gain_ref,
    w0_raw,
    w2_raw,
    w0,
    w1,
    w2,
    expand,
    rot_scr,
    entries,
    mult,
    single,
    xg,
    turned,
    part_scr,
    y_scr,
    msg,
    recv,
    rrot,
    f_scr,
    back,
    sq,
    sq_other,
    wsem,
    esem,
    rot_sem,
    msg_sem,
    qsem,
):
    me = lax.axis_index("dev")
    half = lax.axis_index("rep")
    nodes = x_ref.shape[0]
    flat = x_ref.shape[1]
    blocks = peers * slots // BLOCK
    group = BLOCK // slots
    partner = {"rep": 1 - half}

    side = lax.div(me, peers // 2)

    def peer(index):
        index = lax.rem(index + half * (peers - 1 - peers // 2), peers - 1)
        step, odd = index // 2, index % 2
        mixed = (1 - odd) * step + odd * (peers - 2 - step)
        index = side * index + (1 - side) * mixed
        return index + lax.div(index + peers - me, peers)

    def load(index, src, dst):
        return pltpu.make_async_copy(src, dst, wsem.at[index])

    early = [
        load(0, rot_hbm, rot_ref),
        load(1, src_hbm, src_ref),
        load(2, cnt_hbm, cnt_ref),
        load(3, x_hbm, x_ref),
    ]
    late = []
    width = w1_hbm.shape[-1]
    for part in (0, 1):
        for kind in (0, 1):
            cols = slice(kind * width, (kind + 1) * width)
            late.append(load(7, w1_hbm.at[kind, :, part], w1.at[part, :, :, cols]))
    late += [
        load(5, w0_hbm, w0_raw),
        load(6, w2_hbm, w2_raw),
        load(4, dst_hbm, dst_ref),
        load(8, gain_hbm, gain_ref),
    ]
    for copy in (early[3], *early[:3]):
        copy.start()
    barrier = pltpu.get_barrier_semaphore()
    pl.semaphore_signal(barrier, inc=1, device_id=partner, device_id_type=MESH)
    each(
        peers - 1,
        lambda o: pl.semaphore_signal(
            barrier, inc=1, device_id={"dev": peer(o)}, device_id_type=MESH
        ),
    )

    def lanes(rows):
        return lax.broadcasted_iota(jnp.int32, (rows, LANES), 1)

    y_scr[...] = jnp.zeros_like(y_scr)
    xg[:, flat:] = jnp.zeros((BLOCK, xg.shape[1] - flat), jnp.float32)
    for window in (0, 1):
        entry = lax.broadcasted_iota(jnp.int32, (LANES, LANES), 0) + window * LANES
        spot = lax.broadcasted_iota(jnp.int32, (LANES, LANES), 1)
        shift = jnp.zeros_like(entry)
        for start, offset in SEGMENTS:
            shift = jnp.where(entry >= start, offset, shift)
        place = lax.rem(entry + shift, 4)
        for part in (0, 1):
            hit = place == lax.div(spot, HALF) + 2 * part
            expand[window, :, part * LANES : (part + 1) * LANES] = jnp.where(
                hit, 1.0, 0.0
            ).astype(jnp.bfloat16)

    for copy in late:
        copy.start()

    def column(rows):
        row = lax.broadcasted_iota(jnp.int32, (BLOCK, group), 0)
        spot = lax.broadcasted_iota(jnp.int32, (BLOCK, group), 1)
        chosen = jnp.zeros((BLOCK, group), jnp.float32)
        for index in range(slots):
            chosen = jnp.where(row == spot * slots + index, rows[index], chosen)
        return jnp.sum(chosen, axis=1, keepdims=True)

    def sources(block):
        count = cnt_ref[block]
        value = src_ref[block]
        return column(
            [
                jnp.where(count > index, value[index : index + 1], -1).astype(jnp.float32)
                for index in range(slots)
            ]
        )

    def targets(block):
        value = dst_ref[block].astype(jnp.float32)
        down = column([value[index : index + 1] for index in range(slots)])
        row = lax.broadcasted_iota(jnp.int32, (BLOCK, BLOCK), 0)
        spot = lax.broadcasted_iota(jnp.int32, (BLOCK, BLOCK), 1)
        return jnp.sum(jnp.where(row == spot, down, 0.0), axis=0, keepdims=True)

    def place(ref, start, edges, spot=0):
        base = spot * edges
        for index in range(edges // slots):
            first = base + index * slots
            rot_scr[first : first + slots, 0:ROT] = ref[start + index].astype(jnp.float32)
        for number, (window, first, last) in enumerate(GROUPS):
            spots = lanes(edges) + window * LANES
            rows = rot_scr[base : base + edges, window * LANES : (window + 1) * LANES]
            first_row = (spot * len(GROUPS) + number) * edges
            entries[first_row : first_row + edges, :] = jnp.where(
                (spots >= first) & (spots <= last), rows, 0.0
            ).astype(jnp.bfloat16)

    def spread(edges, spot=0, windows=(0, 1), cuts=1):
        base = spot * edges
        for window in windows:
            first = LOW_GROUPS * window
            count = len(GROUPS) - LOW_GROUPS if window else LOW_GROUPS
            edge = [first + count * step // cuts for step in range(cuts + 1)]
            for start, end in zip(edge[:-1], edge[1:]):
                span = slice(
                    (spot * len(GROUPS) + start) * edges, (spot * len(GROUPS) + end) * edges
                )
                mult[span] = jnp.dot(
                    entries[span], expand[window], preferred_element_type=jnp.float32
                )
        if 0 not in windows:
            return
        for number, entry in enumerate(ALONE):
            value = rot_scr[base : base + edges, entry : entry + 1]
            value = jnp.broadcast_to(value, (edges, LANES))
            first_row = (spot * len(ALONE) + number) * edges
            single[first_row : first_row + edges, :] = jnp.where(
                lanes(edges) < HALF, value, 0.0
            )

    def factor(number, which, edges, spot=0):
        number += spot * len(ALONE if which is None else GROUPS)
        span = slice(number * edges, (number + 1) * edges)
        if which is None:
            return single[span, :]
        return mult[span, which * LANES : (which + 1) * LANES]

    def turn(block):
        low_half = lanes(BLOCK) < HALF
        hot = (
            lax.broadcasted_iota(jnp.int32, (BLOCK, nodes), 1).astype(jnp.float32) == sources(block)
        ).astype(jnp.bfloat16)
        place(rot_ref, block * group, BLOCK)
        spread(BLOCK, windows=(0,), cuts=2)
        if block is first_block:
            early[3].wait()
        spread(BLOCK, windows=(1,), cuts=2)
        xg[:, 0:flat] = jnp.dot(hot, x_ref[...], preferred_element_type=jnp.float32)
        sums = [None] * FRAME
        for slot, tile, number, which in PARTS:
            part = factor(number, which, BLOCK) * xg[:, tile * LANES : (tile + 1) * LANES]
            sums[slot] = part if sums[slot] is None else sums[slot] + part
        for pair, (one, two) in enumerate(PAIRS):
            kept = jnp.where(low_half, sums[one], sums[two])
            moved = jnp.where(low_half, sums[two], sums[one])
            turned[half, block, :, pair * LANES : (pair + 1) * LANES] = (
                kept + pltpu.roll(moved, HALF, 1)
            ).astype(jnp.bfloat16)

    for copy in early[:3]:
        copy.wait()
    first_block = 0 if blocks <= 16 else None
    if first_block is None:
        early[3].wait()
    each(blocks, turn)

    pl.semaphore_wait(barrier, peers)

    exchange = pltpu.make_async_remote_copy(
        src_ref=turned.at[half],
        dst_ref=turned.at[half],
        send_sem=esem.at[0],
        recv_sem=esem.at[1],
        device_id=partner,
        device_id_type=MESH,
    )
    exchange.start()

    def transfer(source, target, sems, o):
        to = peer(o)
        return pltpu.make_async_remote_copy(
            src_ref=source.at[to],
            dst_ref=target.at[me],
            send_sem=sems.at[2],
            recv_sem=sems.at[side],
            device_id={"dev": to},
            device_id_type=MESH,
        )

    def keep(source, target, sems):
        return pltpu.make_async_copy(source.at[me], target.at[me], sems.at[side])

    def arrived(target, sems, part):
        span = target.at[pl.ds(part * (peers // 2), peers // 2)]
        return pltpu.make_async_copy(span, span, sems.at[part])

    def sent(source, sems):
        span = source.at[pl.ds(0, peers - 1)]
        return pltpu.make_async_copy(span, span, sems.at[2])

    each(peers - 1, lambda o: transfer(rot_ref, rrot, rot_sem, o).start())
    keep(rot_ref, rrot, rot_sem).start()

    def rows(part, block, order):
        start = STARTS[order]
        return turned[part, block, :, start : start + ORDERS[order][1] * HALF]

    def product(part, block, order):
        if order == 0:
            lhs = rows(part, block, order)
            return [(0, jnp.dot(lhs, w0[part], preferred_element_type=jnp.float32))]
        lhs = jnp.concatenate(
            [rows(part, block, order), rows(part, block, order + 1)], axis=0
        )
        rhs, gap = (w1[part], width) if order == 1 else (w2[part], SPLIT)
        if rhs.ndim == 3:
            rhs = rhs.reshape(-1, rhs.shape[-1])
        both = jnp.dot(lhs, rhs, preferred_element_type=jnp.float32)
        span = ORDERS[order][1] * HALF
        plus = both[:BLOCK, :span] - both[BLOCK:, gap : gap + span]
        minus = both[:BLOCK, gap : gap + span] + both[BLOCK:, :span]
        return [(order, plus), (order + 1, minus)]

    def own(order):
        def one(block):
            for spot, value in product(half, block, order):
                start = STARTS[spot]
                part_scr[block, :, start : start + value.shape[1]] = value

        return one

    load(7, w1, w1).wait()
    late[4].wait()
    for slot in range(ORDERS[0][1]):
        flipped = w0_raw[:, slot * LANES : (slot + 1) * LANES].T
        for part in (0, 1):
            w0[part, slot * HALF : (slot + 1) * HALF, :] = flipped[part * HALF : (part + 1) * HALF]
    each(blocks, own(1))
    late[5].wait()
    for kind in (0, 1):
        for slot in range(ORDERS[3][1]):
            flipped = w2_raw[kind, :, slot * LANES : (slot + 1) * LANES].T
            for part in (0, 1):
                w2[
                    part,
                    slot * HALF : (slot + 1) * HALF,
                    kind * SPLIT : kind * SPLIT + flipped.shape[1],
                ] = flipped[part * HALF : (part + 1) * HALF]
    each(blocks, own(0))
    each(blocks, own(3))

    def mix(block):
        values = []
        for order in (3, 1, 0):
            values += product(1 - half, block, order)
        for spot, value in values:
            start = STARTS[spot]
            sent = SENT[spot]
            y_scr[:, sent : sent + value.shape[1]] = (
                value + part_scr[block, :, start : start + value.shape[1]]
            )
        for index in range(group):
            msg[block * group + index] = y_scr[index * slots : (index + 1) * slots, :].astype(
                jnp.bfloat16
            )

    exchange.wait_recv()
    each(blocks, mix)
    each(peers - 1, lambda o: transfer(msg, recv, msg_sem, o).start())
    keep(msg, recv, msg_sem).start()

    def collect(start, spot=0):
        low_half = lanes(PIECE) < HALF
        for index in range(PIECE // slots):
            f_scr[index * slots : (index + 1) * slots, :] = recv[start + index].astype(jnp.float32)
        doubled = {}
        for slot in range(FRAME):
            tile, side = message_place(slot)
            value = f_scr[:, tile * LANES : (tile + 1) * LANES]
            turned = pltpu.roll(value, HALF, 1)
            doubled[slot] = (
                jnp.where(low_half, value, turned) if side == 0 else jnp.where(low_half, turned, value)
            )
        sums = [None] * TILES
        for slot, tile, number, which in PARTS:
            part = factor(number, which, PIECE, spot) * doubled[slot]
            sums[tile] = part if sums[tile] is None else sums[tile] + part
        first = pl.multiple_of(start * slots, PIECE)
        for tile in range(TILES):
            back[pl.ds(first, PIECE), tile * LANES : (tile + 1) * LANES] = sums[tile].astype(
                jnp.bfloat16
            )

    wide = PIECE // slots
    pieces = peers // 2 // wide
    late[6].wait()
    late[7].wait()
    if pieces == 1:
        for part in (0, 1):
            arrived(rrot, rot_sem, part).wait()
            place(rrot, part * wide, PIECE, part)
            spread(PIECE, part)
        for part in (0, 1):
            arrived(recv, msg_sem, part).wait()
            collect(part * wide, part)
    else:
        for part in (0, 1):
            arrived(rrot, rot_sem, part).wait()
            arrived(recv, msg_sem, part).wait()
            base = part * (peers // 2)

            def one(piece, carry):
                place(rrot, base + piece * wide, PIECE)
                spread(PIECE)
                collect(base + piece * wide)
                return carry

            lax.fori_loop(0, pieces, one, 0)

    hot = jnp.concatenate(
        [
            (
                lax.broadcasted_iota(jnp.int32, (nodes, BLOCK), 0).astype(jnp.float32)
                == targets(block)
            ).astype(jnp.bfloat16)
            for block in range(blocks)
        ],
        axis=1,
    )
    partial = None
    for start in range(0, WIDE, 2 * LANES):
        cols = slice(start, min(start + 2 * LANES, WIDE))
        value = jnp.dot(hot, back[:, cols], preferred_element_type=jnp.float32)
        total[:, cols] = value
        for part in range(0, cols.stop - start, LANES):
            square = value[:, part : part + LANES] * value[:, part : part + LANES]
            partial = square if partial is None else partial + square
    sq[...] = partial
    share = pltpu.make_async_remote_copy(
        src_ref=sq,
        dst_ref=sq_other,
        send_sem=qsem.at[0],
        recv_sem=qsem.at[1],
        device_id=partner,
        device_id_type=MESH,
    )
    share.start()
    for start in range(0, flat, LANES):
        cols = slice(start, min(start + LANES, flat))
        total[:, cols] = total[:, cols] * gain_ref[:, cols]
    exchange.wait_send()
    sent(rot_ref, rot_sem).wait()
    sent(msg, msg_sem).wait()
    share.wait()
    sums_ref[...] = sq[...] + sq_other[...]


def finish(chunks, x_ref, total, sums_ref, out_hbm, out_ref, sems):
    flat = x_ref.shape[1]
    mean_sq = jnp.sum(sums_ref[...], axis=1, keepdims=True) / (2 * flat)
    scale = lax.rsqrt(mean_sq + 1e-06)
    copies = []
    for index, (first, last) in enumerate(chunks):
        for start in range(first, last, LANES):
            cols = slice(start, min(start + LANES, last))
            normed = total[:, cols] * scale
            out_ref[:, cols] = (x_ref[:, cols].astype(jnp.float32) + normed).astype(jnp.bfloat16)
        part = slice(first, last)
        copies.append(
            pltpu.make_async_copy(out_ref.at[:, part], out_hbm.at[:, part], sems.at[index])
        )
        copies[-1].start()
    for copy in copies:
        copy.wait()


def shards(node_features, src_node, dst_node, counts, rotation, w_zero, w_one, w_two, norm_gain):
    nodes, _, flat = node_features.shape
    peers, slots = src_node.shape[1:]
    edges = peers * slots
    blocks = edges // BLOCK
    x = node_features.reshape(nodes, flat)
    group = peers // blocks
    src = src_node.reshape(blocks, group, slots).swapaxes(1, 2)
    dst = dst_node.reshape(blocks, group, slots).swapaxes(1, 2)
    cnt = counts.reshape(blocks, 1, group)
    rot = rotation.reshape(peers, slots, ROT)
    w0 = w_zero.reshape(w_zero.shape[0], -1).T
    w1 = w_one.reshape(2, -1, 2, HALF, w_one.shape[-1])
    w2 = w_two.reshape(2, w_two.shape[1], -1).swapaxes(1, 2)
    vmem = pl.BlockSpec(memory_space=pltpu.VMEM)
    hbm = pl.BlockSpec(memory_space=pltpu.HBM)
    f32, bf16 = jnp.float32, jnp.bfloat16
    dma = pltpu.SemaphoreType.DMA
    operands = (x, rot, src, cnt, dst, norm_gain, w0, w1, w2)
    held, total, sums = pl.pallas_call(
        functools.partial(kernel, peers, slots),
        out_shape=(
            jax.ShapeDtypeStruct((nodes, flat), bf16),
            jax.ShapeDtypeStruct((nodes, WIDE), f32),
            jax.ShapeDtypeStruct((nodes, LANES), f32),
        ),
        in_specs=[hbm] * 9,
        out_specs=(vmem,) * 3,
        scratch_shapes=[
            pltpu.VMEM(rot.shape, bf16),
            pltpu.VMEM(src.shape, jnp.int32),
            pltpu.VMEM(cnt.shape, jnp.int32),
            pltpu.VMEM(dst.shape, jnp.int32),
            pltpu.VMEM(norm_gain.shape, f32),
            pltpu.VMEM(w0.shape, bf16),
            pltpu.VMEM(w2.shape, bf16),
            pltpu.VMEM((2, w0.shape[1] // 2, w0.shape[0]), bf16),
            pltpu.VMEM((2, w1.shape[1], HALF, 2 * w1.shape[-1]), bf16),
            pltpu.VMEM((2, w2.shape[2] // 2, 2 * SPLIT), bf16),
            pltpu.VMEM((2, LANES, 2 * LANES), bf16),
            pltpu.VMEM((BLOCK, 2 * LANES), f32),
            pltpu.VMEM((ALL_ROWS, LANES), bf16),
            pltpu.VMEM((ALL_ROWS, 2 * LANES), f32),
            pltpu.VMEM((BLOCK * len(ALONE), LANES), f32),
            pltpu.VMEM((BLOCK, WIDE), f32),
            pltpu.VMEM((2, blocks, BLOCK, len(PAIRS) * LANES), bf16),
            pltpu.VMEM((blocks, BLOCK, len(PAIRS) * LANES), f32),
            pltpu.VMEM((BLOCK, MESSAGE), f32),
            pltpu.VMEM((peers, slots, MESSAGE), bf16),
            pltpu.VMEM((peers, slots, MESSAGE), bf16),
            pltpu.VMEM((peers, slots, ROT), bf16),
            pltpu.VMEM((PIECE, MESSAGE), f32),
            pltpu.VMEM((edges, WIDE), bf16),
            pltpu.VMEM((nodes, LANES), f32),
            pltpu.VMEM((nodes, LANES), f32),
            dma((9,)),
            dma((2,)),
            dma((3,)),
            dma((3,)),
            dma((2,)),
        ],
        compiler_params=pltpu.CompilerParams(
            collective_id=0, has_side_effects=True, vmem_limit_bytes=VMEM_LIMIT
        ),
    )(*(pltpu.with_memory_space_constraint(operand, pltpu.HBM) for operand in operands))
    cut = (flat // LANES + 3) // 4 * LANES
    chunks = [(start, min(start + cut, flat)) for start in range(0, flat, cut)]
    out = pl.pallas_call(
        functools.partial(finish, chunks),
        out_shape=jax.ShapeDtypeStruct((nodes, flat), bf16),
        in_specs=[vmem] * 3,
        out_specs=hbm,
        scratch_shapes=[pltpu.VMEM((nodes, flat), bf16), dma((len(chunks),))],
        compiler_params=pltpu.CompilerParams(vmem_limit_bytes=VMEM_LIMIT),
    )(held, total, sums)
    return out.reshape(nodes, 1, flat)


def solution(mesh):
    return jax.shard_map(
        shards,
        mesh=mesh,
        in_specs=(
            P("dev", "rep", None),
            P("dev", None, None),
            P("dev", None, None),
            P("dev", None),
            P("dev", None, None, None),
            P(None, "rep", None),
            P(None, None, "rep", None),
            P(None, None, "rep", None),
            P("rep", None),
        ),
        out_specs=P("dev", "rep", None),
        check_vma=False,
    )
```
